128 devices in a mesh: data: 1, dap: 128 (over z, y, x, core).
Axes of the slice: x: 4, y: 4, z: 4, core: 2. Of those that a mesh axis runs over, the one named last changes fastest.
Arguments:
- z: bfloat16 [1536, 1536, 128], P(('data', 'dap'))
- mask: int32 [1536, 1536], P(('data', 'dap'))
- ln_scale: bfloat16 [128], replicated
- ln_bias: bfloat16 [128], replicated
- w_a: bfloat16 [128, 128], replicated
- w_a_gate: bfloat16 [128, 128], replicated
- w_b: bfloat16 [128, 128], replicated
- w_b_gate: bfloat16 [128, 128], replicated
- w_gate: bfloat16 [128, 128], replicated
- ln_hid_scale: bfloat16 [128], replicated
- ln_hid_bias: bfloat16 [128], replicated
- w_out: bfloat16 [128, 128], replicated
Outputs:
- output: bfloat16 [1536, 1536, 128], P(('data', 'dap'))
All inputs are finite; a program needn't handle non-finite values.
Results may differ from the reference program's by a relative error of at most 0.00375147.
Values are sent between devices in bfloat16 or wider.
A program may use at most 1 GiB of HBM per device.

```python
import jax
import jax.numpy as jnp
from jax import lax

CROP_LEN = 1536
PAIR_CH = 128
HIDDEN_CH = 128
LN_EPS = 1e-5


def layer_norm(vals, scale, bias):
    mean_val = jnp.mean(vals, axis=-1, keepdims=True)
    centered = vals - mean_val
    variance = jnp.mean(centered * centered, axis=-1, keepdims=True)
    return centered * lax.rsqrt(variance + LN_EPS) * scale + bias


def setup_inputs(seed: int = 0, part: int = 0) -> dict:
    base_key = jax.random.key(seed)
    part_key = jax.random.fold_in(base_key, part)
    key_z, key_mask = jax.random.split(part_key, 2)
    weight_keys = jax.random.split(base_key, 10)

    def draw_normal(key_idx, shape, scale):
        return jax.random.normal(weight_keys[key_idx], shape, jnp.float32) * scale

    z_vals = jax.random.normal(key_z, (CROP_LEN, CROP_LEN, PAIR_CH), jnp.float32)
    keep_res = (jax.random.randint(key_mask, (CROP_LEN,), 0, 16) != 0).astype(jnp.int32)
    pair_mask = keep_res[:, None] * keep_res[None, :]
    pair_scale = PAIR_CH ** -0.5
    hid_scale = HIDDEN_CH ** -0.5
    return {
        'z': z_vals.astype(jnp.bfloat16),
        'mask': pair_mask,
        'ln_scale': (1.0 + draw_normal(0, (PAIR_CH,), 0.25)).astype(jnp.bfloat16),
        'ln_bias': draw_normal(1, (PAIR_CH,), 0.1).astype(jnp.bfloat16),
        'w_a': draw_normal(2, (PAIR_CH, HIDDEN_CH), pair_scale).astype(jnp.bfloat16),
        'w_a_gate': draw_normal(3, (PAIR_CH, HIDDEN_CH), pair_scale).astype(jnp.bfloat16),
        'w_b': draw_normal(4, (PAIR_CH, HIDDEN_CH), pair_scale).astype(jnp.bfloat16),
        'w_b_gate': draw_normal(5, (PAIR_CH, HIDDEN_CH), pair_scale).astype(jnp.bfloat16),
        'w_gate': draw_normal(6, (PAIR_CH, PAIR_CH), pair_scale).astype(jnp.bfloat16),
        'ln_hid_scale': (1.0 + draw_normal(7, (HIDDEN_CH,), 0.25)).astype(jnp.bfloat16),
        'ln_hid_bias': draw_normal(8, (HIDDEN_CH,), 0.25).astype(jnp.bfloat16),
        'w_out': draw_normal(9, (HIDDEN_CH, PAIR_CH), 2.0 * hid_scale).astype(jnp.bfloat16),
    }


def reference(z, mask, ln_scale, ln_bias, w_a, w_a_gate, w_b, w_b_gate, w_gate, ln_hid_scale, ln_hid_bias, w_out):
    w_cat = jnp.concatenate([w_a, w_a_gate, w_b, w_b_gate], axis=1)

    def norm_rows(z_row):
        return layer_norm(z_row.astype(jnp.float32), ln_scale, ln_bias).astype(jnp.bfloat16)

    def row_proj(row_args):
        z_row, mask_row = row_args
        projected = jnp.dot(norm_rows(z_row), w_cat, preferred_element_type=jnp.float32)
        proj_a, gate_a, proj_b, gate_b = jnp.split(projected, 4, axis=1)
        mask_col = mask_row.astype(jnp.float32)[:, None]
        a_row = (mask_col * jax.nn.sigmoid(gate_a) * proj_a).astype(jnp.bfloat16)
        b_row = (mask_col * jax.nn.sigmoid(gate_b) * proj_b).astype(jnp.bfloat16)
        return a_row, b_row

    a_rows, b_rows = lax.map(row_proj, (z, mask))
    a_chan = jnp.transpose(a_rows, (2, 0, 1))
    b_chan = jnp.transpose(b_rows, (2, 0, 1))

    def chan_prod(chan_args):
        a_mat, b_mat = chan_args
        return jnp.dot(a_mat, b_mat.T, preferred_element_type=jnp.float32).astype(jnp.bfloat16)

    tri_chan = lax.map(chan_prod, (a_chan, b_chan))
    tri_rows = jnp.transpose(tri_chan, (1, 2, 0))

    def row_out(row_args):
        z_row, t_row = row_args
        y_row = layer_norm(t_row.astype(jnp.float32), ln_hid_scale, ln_hid_bias).astype(jnp.bfloat16)
        update = jnp.dot(y_row, w_out, preferred_element_type=jnp.float32)
        gate_val = jax.nn.sigmoid(jnp.dot(norm_rows(z_row), w_gate, preferred_element_type=jnp.float32))
        return (z_row.astype(jnp.float32) + gate_val * update).astype(jnp.bfloat16)

    return lax.map(row_out, (z, tri_rows))
```

```python
import functools

import jax
import jax.numpy as jnp
from jax import lax
from jax.experimental import pallas as pl
from jax.experimental.pallas import tpu as pltpu
from jax.sharding import PartitionSpec as P

LN_EPS = 1e-5
MESH = pl.DeviceIdType.MESH
DMA = pltpu.SemaphoreType.DMA
VMEM = pltpu.VMEM
ANY = pl.ANY
N = 1536
C = 128
SIDE = 4
CH = 64
RL = 12
TR = 8
NG = 3
KC = 256
HALF = N // 2
SKEW = 9
YSK = 129
BF = jnp.bfloat16
F32 = jnp.float32


def place():
    me = lax.axis_index('dap')
    chip, core = me // 2, me % 2
    return core, (chip // 16, (chip // 4) % 4, chip % 4)


def dev(coords, core):
    return {'dap': (coords[0] * 16 + coords[1] * 4 + coords[2]) * 2 + core}


def shift(coords, dim, by):
    return tuple((v + by) % SIDE if i == dim else v for i, v in enumerate(coords))


def pick(dim, at):
    return tuple(at if i == dim else slice(None) for i in range(3))


def enter(core, coords):
    barrier = pltpu.get_barrier_semaphore()
    for dim in range(3):
        for by in range(1, SIDE):
            pl.semaphore_signal(barrier, inc=1, device_id=dev(shift(coords, dim, by), core), device_id_type=MESH)
    pl.semaphore_signal(barrier, inc=1, device_id=dev(coords, 1 - core), device_id_type=MESH)
    pl.semaphore_wait(barrier, 3 * (SIDE - 1) + 1)


def wait_bytes(ref, sem):
    pltpu.make_async_copy(ref, ref, sem).wait()


def send_phase(core, coords, dim, src_at, dst_at, ssem, rsem):
    for by in (1, 3, 2):
        to = (coords[dim] + by) % SIDE
        pltpu.make_async_remote_copy(
            src_ref=src_at(pick(dim, to)), dst_ref=dst_at(pick(dim, coords[dim])), send_sem=ssem, recv_sem=rsem,
            device_id=dev(shift(coords, dim, by), core), device_id_type=MESH).start()


def keep_own(coords, dim, src, dst, lead):
    def body(i, carry):
        idx = [i // SIDE, i % SIDE]
        idx.insert(dim, coords[dim])
        at = lead + tuple(idx)
        dst[at] = src[at]
        return carry
    lax.fori_loop(0, SIDE * SIDE, body, 0)


def sigmoid(v):
    return 0.5 * jnp.tanh(0.5 * v) + 0.5


def pairs_kernel(z_hbm, mask_ref, scale_ref, bias_ref, wa_ref, wag_ref, wb_ref, wbg_ref, b_out, a_out, x_out,
                 zbuf, xall, mall, wt, stage_a, stage_b, sa, sb, r1a, r1b, r2a, r2b,
                 zsem, xssem, xrsem, mrsem, msem, xosem, ssem, rsem, fsem):
    core, coords = place()
    for r in range(RL):
        pltpu.make_async_copy(z_hbm.at[r], zbuf.at[r], zsem.at[r]).start()
    for i, w in enumerate((wa_ref, wag_ref, wb_ref, wbg_ref)):
        wt[i] = w[...].astype(F32).T.astype(BF)
    mall[core] = mask_ref[...]
    enter(core, coords)
    partner = dev(coords, 1 - core)
    mcopy = pltpu.make_async_remote_copy(src_ref=mask_ref, dst_ref=mall.at[core], send_sem=msem, recv_sem=mrsem,
                                         device_id=partner, device_id_type=MESH)
    mcopy.start()
    scale = scale_ref[...].astype(F32)
    bias = bias_ref[...].astype(F32)

    def norm_row(r, carry):
        wait_bytes(zbuf.at[0], zsem.at[r])
        row = core * RL + r

        def chunk(i, carry):
            at = pl.ds(pl.multiple_of(i * KC, KC), KC)
            v = zbuf[r, at, :].astype(F32)
            centered = v - jnp.mean(v, axis=-1, keepdims=True)
            var = jnp.mean(centered * centered, axis=-1, keepdims=True)
            xall[row, at, :] = (centered * lax.rsqrt(var + LN_EPS) * scale + bias).astype(BF)
            return carry
        lax.fori_loop(0, N // KC, chunk, 0)
        pltpu.make_async_remote_copy(src_ref=xall.at[row], dst_ref=xall.at[row], send_sem=xssem, recv_sem=xrsem.at[r],
                                     device_id=partner, device_id_type=MESH).start()
        pltpu.make_async_copy(xall.at[row], x_out.at[r], xosem).start()
        return carry
    lax.fori_loop(0, RL, norm_row, 0)
    mcopy.wait()

    half = pl.ds(pl.multiple_of(core * CH, CH), CH)
    wcat = jnp.concatenate([wt[i, half, :] for i in range(4)], axis=0)
    send = [(sb, r1b, r2b, 0), (sa, r1a, r2a, 1)]

    def phase(arr, g, ph):
        s, r1, r2, k = send[arr]
        dim = (g + ph) % 3
        src = (s, r1, r2)[ph]
        if ph < 2:
            dst = (r1, r2)[ph]
            send_phase(core, coords, dim, lambda p: src.at[(g,) + p], lambda p: dst.at[(g,) + p], ssem, rsem.at[k, g, ph])
            keep_own(coords, dim, src, dst, (g,))
        else:
            def final(p):
                return b_out.at[p + (g,)] if k == 0 else a_out.at[(g,) + p]
            send_phase(core, coords, dim, lambda p: src.at[(g,) + p], final, ssem, rsem.at[k, g, ph])
            own = pick(dim, coords[dim])
            pltpu.make_async_copy(src.at[(g,) + own], final(own), fsem).start()

    def arrived(arr, g, ph):
        s, r1, r2, k = send[arr]
        wait_bytes(r1.at[g, pl.ds(0, 3)], rsem.at[k, g, ph])

    for g in range(NG):
        def project_row(i, carry):
            row = g * TR + i
            owner, within = row // RL, row % RL

            @pl.when(owner != core)
            def _():
                wait_bytes(xall.at[0], xrsem.at[within])

            for j in range(N // KC):
                at = pl.ds(j * KC, KC)
                p = lax.dot_general(wcat, xall[row, at, :], (((1,), (1,)), ((), ())), preferred_element_type=F32)
                keep = mall[owner, pl.ds(within, 1), at].astype(F32)
                a = sigmoid(p[CH:2 * CH]) * p[:CH] * keep
                b = sigmoid(p[3 * CH:]) * p[2 * CH:3 * CH] * keep
                for t in range(KC // 128):
                    lanes = slice(t * 128, (t + 1) * 128)
                    kt = j * (KC // 128) + t
                    stage_a[kt, pl.ds(i, CH, stride=SKEW), :] = a[:, lanes]
                    stage_b[kt, pl.ds(i, CH, stride=SKEW), :] = b[:, lanes]
            return carry
        lax.fori_loop(0, TR, project_row, 0)

        def pack(c, carry):
            at = (g, c // 16, (c // 4) % 4, c % 4)
            for stage, s in ((stage_b, sb), (stage_a, sa)):
                for j in range(N // KC):
                    v = jnp.concatenate([stage[2 * j + t, pl.ds(c * SKEW, TR), :] for t in range(2)], axis=1)
                    s[at + (slice(None), pl.ds(j * KC, KC))] = v.astype(BF)
            return carry
        lax.fori_loop(0, CH, pack, 0)
        phase(0, g, 0)

    for g in range(NG):
        phase(1, g, 0)
    for ph in (1, 2):
        for arr in range(2):
            for g in range(NG):
                arrived(arr, g, ph - 1)
                phase(arr, g, ph)
    for arr in range(2):
        for g in range(NG):
            arrived(arr, g, 2)
    for _ in range(6):
        wait_bytes(r1a.at[:, pl.ds(0, 3)], ssem)
    for _ in range(2):
        wait_bytes(r1a.at[:, 0], fsem)
    wait_bytes(zbuf, xosem)
    wait_bytes(zbuf, xssem)


def triangle_kernel(a_hbm, b_hbm, own_out, par_out, abuf, bbuf, t, r1, r2, lsem, ssem, rsem, fsem, dssem, drsem):
    core, coords = place()
    bcopy = pltpu.make_async_copy(b_hbm, bbuf, lsem.at[NG])
    acopy = [pltpu.make_async_copy(a_hbm.at[g], abuf.at[g], lsem.at[g]) for g in range(NG)]
    bcopy.start()
    for cp in acopy:
        cp.start()
    enter(core, coords)
    bcopy.wait()

    def phase(g, h, ph):
        dim = (g + ph) % 3
        src = (t, r1, r2)[ph]
        if ph < 2:
            dst = (r1, r2)[ph]
            send_phase(core, coords, dim, lambda p: src.at[(g, h) + p], lambda p: dst.at[(g, h) + p], ssem, rsem.at[g, h, ph])
            keep_own(coords, dim, src, dst, (g, h))
        else:
            def final(p):
                return own_out.at[p + (g, slice(None), pl.ds(h * HALF, HALF))]
            send_phase(core, coords, dim, lambda p: src.at[(g, h) + p], final, ssem, rsem.at[g, h, ph])
            own = pick(dim, coords[dim])
            pltpu.make_async_copy(src.at[(g, h) + own], final(own), fsem.at[h]).start()

    def arrived(g, h, ph):
        wait_bytes(r1.at[g, h, pl.ds(0, 3)], rsem.at[g, h, ph])

    for h in range(2):
        for g in range(NG):
            if h == 0:
                acopy[g].wait()

            for n in range(HALF // KC):
                acc = lax.dot_general(abuf[g], bbuf[pl.ds(h * HALF + n * KC, KC), :], (((1,), (1,)), ((), ())),
                                      preferred_element_type=F32)
                t[g, h, :, :, :, :, pl.ds(n * KC, KC)] = acc.astype(BF).reshape(SIDE, SIDE, SIDE, TR, KC)
            phase(g, h, 0)
    for ph in (1, 2):
        for h in range(2):
            for g in range(NG):
                arrived(g, h, ph - 1)
                phase(g, h, ph)
    swaps = []
    for h in range(2):
        for g in range(NG):
            arrived(g, h, 2)
        wait_bytes(r1.at[:, 0, 0], fsem.at[h])
        cols = pl.ds(h * HALF, HALF)
        swap = pltpu.make_async_remote_copy(
            src_ref=own_out.at[:, :, :, pl.ds(1 - core, 2), :, cols], dst_ref=par_out.at[:, :, :, :, :, cols],
            send_sem=dssem.at[h], recv_sem=drsem.at[h], device_id=dev(coords, 1 - core), device_id_type=MESH)
        swap.start()
        swaps.append(swap)
    for swap in swaps:
        swap.wait()
    for _ in range(3):
        wait_bytes(r1.at[:, :, pl.ds(0, 3)], ssem)


def finish_kernel(hid_ref, town, tpar, x_ref, z_ref, wg_ref, wo_ref, out_ref, y):
    core = lax.axis_index('dap') % 2
    step = 8

    def own(c):
        return town[pl.ds(c, step), pl.ds(core, 2), :, :].astype(F32)

    def par(c):
        return tpar[pl.ds(c, step), :, :, :].astype(F32)

    def add(i, acc):
        c = i * step
        return acc + jnp.sum(own(c), axis=0) + jnp.sum(par(c), axis=0)
    zero = jnp.zeros((2, TR, KC), F32)
    mean = lax.fori_loop(0, CH // step, add, zero) * (1.0 / C)

    def add_sq(i, acc):
        c = i * step
        u, v = own(c) - mean, par(c) - mean
        return acc + jnp.sum(u * u, axis=0) + jnp.sum(v * v, axis=0)
    var = lax.fori_loop(0, CH // step, add_sq, zero) * (1.0 / C)
    rstd = lax.rsqrt(var + LN_EPS)

    def spread(i, carry):
        for first, vals in ((core * CH, own(i * step)), ((1 - core) * CH, par(i * step))):
            for k in range(step):
                c = first + i * step + k
                v = (vals[k] - mean) * rstd * hid_ref[0, c] + hid_ref[1, c]
                for tile in range(2):
                    for lt in range(KC // 128):
                        y[lt, pl.ds(tile * TR * YSK + c, TR, stride=YSK), :] = v[tile, :, lt * 128:(lt + 1) * 128]
        return carry
    lax.fori_loop(0, CH // step, spread, 0)

    def row(r, carry):
        at = pl.ds((r + 4 * core) * YSK, C)
        yt = jnp.concatenate([y[lt, at, :] for lt in range(KC // 128)], axis=1).astype(BF)
        update = lax.dot_general(yt, wo_ref[...], (((0,), (0,)), ((), ())), preferred_element_type=F32)
        gate = sigmoid(jnp.dot(x_ref[r], wg_ref[...], preferred_element_type=F32))
        out_ref[r] = (z_ref[r].astype(F32) + gate * update).astype(BF)
        return carry
    lax.fori_loop(0, RL, row, 0)


def solution(mesh):
    row_spec = P(('data', 'dap'), None, None)
    mask_spec = P(('data', 'dap'), None)
    replicated = P()
    vspec = pl.BlockSpec(memory_space=VMEM)
    aspec = pl.BlockSpec(memory_space=ANY)

    def local_fn(z_loc, mask_loc, ln_scale, ln_bias, w_a, w_a_gate, w_b, w_b_gate, w_gate, ln_hid_scale, ln_hid_bias, w_out):
        sets = (NG, SIDE, SIDE, SIDE, TR, N)
        chips = (SIDE, SIDE, SIDE, NG, TR, N)
        b_all, a_all, x_norm = pl.pallas_call(
            pairs_kernel, name='pairs',
            out_shape=(jax.ShapeDtypeStruct(chips, BF), jax.ShapeDtypeStruct(sets, BF), jax.ShapeDtypeStruct((RL, N, C), BF)),
            in_specs=[aspec] + [vspec] * 7, out_specs=(aspec,) * 3,
            scratch_shapes=[
                VMEM((RL, N, C), BF), VMEM((2 * RL, N, C), BF), VMEM((2, RL, N), jnp.int32), VMEM((4, C, C), BF),
                VMEM((N // 128, CH * SKEW, 128), F32), VMEM((N // 128, CH * SKEW, 128), F32),
                VMEM(sets, BF), VMEM(sets, BF), VMEM(sets, BF), VMEM(sets, BF), VMEM(sets, BF), VMEM(sets, BF),
                DMA((RL,)), DMA, DMA((RL,)), DMA, DMA, DMA, DMA, DMA((2, NG, 3)), DMA],
            compiler_params=pltpu.CompilerParams(collective_id=1, has_side_effects=True, vmem_limit_bytes=64 * 2**20 - 65536),
        )(z_loc, mask_loc, ln_scale.reshape(1, C), ln_bias.reshape(1, C), w_a, w_a_gate, w_b, w_b_gate)
        units = (NG, 2, SIDE, SIDE, SIDE, TR, HALF)
        own, par = pl.pallas_call(
            triangle_kernel, name='triangle',
            out_shape=(jax.ShapeDtypeStruct(chips, BF), jax.ShapeDtypeStruct((SIDE, SIDE, SIDE, 2, TR, N), BF)),
            in_specs=[aspec] * 2, out_specs=(aspec,) * 2,
            scratch_shapes=[VMEM((NG, CH * TR, N), BF), VMEM((N, N), BF), VMEM(units, BF), VMEM(units, BF), VMEM(units, BF),
                            DMA((NG + 1,)), DMA, DMA((NG, 2, 3)), DMA((2,)), DMA((2,)), DMA((2,))],
            compiler_params=pltpu.CompilerParams(collective_id=2, has_side_effects=True, vmem_limit_bytes=60 * 2**20),
        )(a_all.reshape(NG, CH * TR, N), b_all.reshape(N, N))
        hid = jnp.stack([ln_hid_scale, ln_hid_bias]).astype(F32)
        wspec = pl.BlockSpec((C, C), lambda j: (0, 0))
        rspec = pl.BlockSpec((RL, KC, C), lambda j: (0, j, 0))
        return pl.pallas_call(
            finish_kernel, name='finish', grid=(N // KC,),
            out_shape=jax.ShapeDtypeStruct((RL, N, C), BF),
            in_specs=[pl.BlockSpec(memory_space=pltpu.SMEM),
                      pl.BlockSpec((CH, NG, TR, KC), lambda j: (0, 0, 0, j)), pl.BlockSpec((CH, 2, TR, KC), lambda j: (0, 0, 0, j)),
                      rspec, rspec, wspec, wspec],
            out_specs=rspec,
            scratch_shapes=[VMEM((KC // 128, 2 * TR * YSK, 128), F32)],
            compiler_params=pltpu.CompilerParams(vmem_limit_bytes=48 * 2**20),
        )(hid, own.reshape(CH, NG, TR, N), par.reshape(CH, 2, TR, N), x_norm, z_loc, w_gate, w_out)

    return jax.shard_map(local_fn, mesh=mesh, in_specs=(row_spec, mask_spec) + (replicated,) * 10, out_specs=row_spec, check_vma=False)
```

```python
import functools

import jax
import jax.numpy as jnp
from jax import lax
from jax.experimental import pallas as pl
from jax.experimental.pallas import tpu as pltpu
from jax.sharding import PartitionSpec as P

LN_EPS = 1e-5
MESH = pl.DeviceIdType.MESH
DMA = pltpu.SemaphoreType.DMA
VMEM = pltpu.VMEM
ANY = pl.ANY
N = 1536
C = 128
SIDE = 4
CH = 64
RL = 12
TR = 8
NG = 3
KC = 256
NT = 3
KT = N // NT
NQ = 4
KQ = N // NQ
SKEW = 9
YSK = 129
BF = jnp.bfloat16
F32 = jnp.float32


def place():
    me = lax.axis_index('dap')
    chip, core = me // 2, me % 2
    return core, (chip // 16, (chip // 4) % 4, chip % 4)


def dev(coords, core):
    return {'dap': (coords[0] * 16 + coords[1] * 4 + coords[2]) * 2 + core}


def shift(coords, dim, by):
    return tuple((v + by) % SIDE if i == dim else v for i, v in enumerate(coords))


def pick(dim, at):
    return tuple(at if i == dim else slice(None) for i in range(3))


def greet(sem, core, coords):
    for dim in range(3):
        for by in range(1, SIDE):
            pl.semaphore_signal(sem, inc=1, device_id=dev(shift(coords, dim, by), core), device_id_type=MESH)
    pl.semaphore_signal(sem, inc=1, device_id=dev(coords, 1 - core), device_id_type=MESH)


GREETED = 3 * (SIDE - 1) + 1


def wait_bytes(ref, sem):
    pltpu.make_async_copy(ref, ref, sem).wait()


def send_phase(core, coords, dim, src_at, dst_at, ssem, rsem):
    for by in (1, 3, 2):
        to = (coords[dim] + by) % SIDE
        pltpu.make_async_remote_copy(
            src_ref=src_at(pick(dim, to)), dst_ref=dst_at(pick(dim, coords[dim])), send_sem=ssem, recv_sem=rsem,
            device_id=dev(shift(coords, dim, by), core), device_id_type=MESH).start()


def keep_own(coords, dim, src, src_at, dst, dst_at):
    def body(i, carry):
        idx = [i // SIDE, i % SIDE]
        idx.insert(dim, coords[dim])
        idx = tuple(idx)
        dst[dst_at(idx)] = src[src_at(idx)]
        return carry
    lax.fori_loop(0, SIDE * SIDE, body, 0)


def sigmoid(v):
    return 0.5 * jnp.tanh(0.5 * v) + 0.5


def update_kernel(hid_ref, z_hbm, mask_ref, scale_ref, bias_ref, wa_ref, wag_ref, wb_ref, wbg_ref, wg_ref, wo_ref, out_hbm,
                  zbuf, xall, mall, wt, stage_a, stage_b, sa, sb, r1a, r1b, r2a, r2b, aa, bb, y, obuf,
                  zsem, xssem, xown, xmix, mrsem, msem, ssem, rsem, tssem, trsem, dssem, drsem, osem, credit):
    core, coords = place()
    barrier = pltpu.get_barrier_semaphore()
    greet(barrier, core, coords)
    partner = dev(coords, 1 - core)
    own0, mix0 = 4 * core, 8 - 8 * core
    tile = [s + core * (2 - 2 * s) for s in range(NG)]
    full = slice(None)

    def kcols(t):
        return pl.ds(t * KT, KT)

    def qcols(q):
        return pl.ds(q * KQ, KQ)

    loads = [pltpu.make_async_copy(z_hbm.at[pl.ds(own0, TR), kcols(t)], zbuf.at[pl.ds(own0, TR), kcols(t)], zsem.at[t])
             for t in range(NT)]
    loads.append(pltpu.make_async_copy(z_hbm.at[pl.ds(mix0, 4)], zbuf.at[pl.ds(mix0, 4)], zsem.at[NT]))
    for cp in loads:
        cp.start()
    for i, w in enumerate((wa_ref, wag_ref, wb_ref, wbg_ref)):
        wt[i] = w[...].astype(F32).T.astype(BF)
    mall[core] = mask_ref[...]
    scale = scale_ref[...].astype(F32)
    bias = bias_ref[...].astype(F32)
    half = pl.ds(pl.multiple_of(core * CH, CH), CH)
    wcat = jnp.concatenate([wt[i, half, :] for i in range(4)], axis=0)

    def norm(first, rows, t):
        def body(i, carry):
            r = first + i
            for k in range(KT // KC):
                at = pl.ds(t * KT + k * KC, KC)
                v = zbuf[r, at, :].astype(F32)
                centered = v - jnp.mean(v, axis=-1, keepdims=True)
                var = jnp.mean(centered * centered, axis=-1, keepdims=True)
                xall[core * RL + r, at, :] = (centered * lax.rsqrt(var + LN_EPS) * scale + bias).astype(BF)
            return carry
        lax.fori_loop(0, rows, body, 0)

    def give_x(first, rows, t, rsem_x):
        block = xall.at[pl.ds(core * RL + first, rows), kcols(t)]
        pltpu.make_async_remote_copy(src_ref=block, dst_ref=block, send_sem=xssem, recv_sem=rsem_x.at[t],
                                     device_id=partner, device_id_type=MESH).start()

    bufs = ((sb, r1b, r2b), (sa, r1a, r2a))

    def phase(arr, s, t, ph):
        dim = (s + t + ph) % 3
        src = bufs[arr][ph]

        def at(p):
            return (s,) + p + (full, kcols(t))

        def final(p):
            return p + (tile[s], full, kcols(t)) if arr == 0 else at(p)
        dst = (bb, aa)[arr] if ph == 2 else bufs[arr][ph + 1]
        dst_at = final if ph == 2 else at
        send_phase(core, coords, dim, lambda p: src.at[at(p)], lambda p: dst.at[dst_at(p)], ssem.at[arr, ph],
                   rsem.at[arr, s, t, ph])
        keep_own(coords, dim, src, at, dst, dst_at)

    def arrived(arr, s, t, ph):
        wait_bytes(r1a.at[s, pl.ds(0, 3), full, full, full, kcols(t)], rsem.at[arr, s, t, ph])

    def make_unit(s, t):
        def project_row(i, carry):
            row = tile[s] * TR + i
            owner, within = row // RL, row % RL
            for j in range(KT // KC):
                at = pl.ds(t * KT + j * KC, KC)
                p = lax.dot_general(wcat, xall[row, at, :], (((1,), (1,)), ((), ())), preferred_element_type=F32)
                keep = mall[owner, pl.ds(within, 1), at].astype(F32)
                a = sigmoid(p[CH:2 * CH]) * p[:CH] * keep
                b = sigmoid(p[3 * CH:]) * p[2 * CH:3 * CH] * keep
                for u in range(KC // 128):
                    lanes = slice(u * 128, (u + 1) * 128)
                    kt = j * (KC // 128) + u
                    stage_a[kt, pl.ds(i, CH, stride=SKEW), :] = a[:, lanes]
                    stage_b[kt, pl.ds(i, CH, stride=SKEW), :] = b[:, lanes]
            return carry
        lax.fori_loop(0, TR, project_row, 0)
        for arr, stage in ((0, stage_b), (1, stage_a)):
            s_ref = bufs[arr][0]

            def pack(c, carry):
                at = (s, c // 16, (c // 4) % 4, c % 4)
                for j in range(KT // KC):
                    v = jnp.concatenate([stage[2 * j + u, pl.ds(c * SKEW, TR), :] for u in range(2)], axis=1)
                    s_ref[at + (full, pl.ds(t * KT + j * KC, KC))] = v.astype(BF)
                return carry
            lax.fori_loop(0, CH, pack, 0, unroll=4)
            phase(arr, s, t, 0)

    for t in range(NT):
        loads[t].wait()
        norm(own0, TR, t)
        if t == 0:
            pl.semaphore_wait(barrier, GREETED)
            mcopy = pltpu.make_async_remote_copy(src_ref=mask_ref, dst_ref=mall.at[core], send_sem=msem, recv_sem=mrsem,
                                                 device_id=partner, device_id_type=MESH)
            mcopy.start()
        give_x(own0, TR, t, xown)
        make_unit(0, t)
    loads[NT].wait()
    for t in range(NT):
        norm(mix0, 4, t)
        give_x(mix0, 4, t, xmix)
    mcopy.wait()
    for s in (1, 2):
        for t in range(NT):
            if s == 1:
                wait_bytes(xall.at[pl.ds(0, 4), kcols(t)], xmix.at[t])
            else:
                wait_bytes(xall.at[pl.ds(0, TR), kcols(t)], xown.at[t])
            make_unit(s, t)

    for ph in (1, 2):
        for arr in range(2):
            for s in range(NG):
                for t in range(NT):
                    arrived(arr, s, t, ph - 1)
                    phase(arr, s, t, ph)
    for arr, ph in ((0, 0), (1, 0), (0, 1), (1, 1), (0, 2)):
        wait_bytes(r1a.at[:, pl.ds(0, 3)], ssem.at[arr, ph])
    greet(credit, core, coords)
    wait_bytes(zbuf, xssem)
    for s in range(NG):
        for t in range(NT):
            arrived(0, s, t, 2)

    def tphase(s, q, ph):
        dim = (s + q + ph) % 3
        src = (sb, r1b, r2b)[ph]
        dst = (r1b, r2b, sa)[ph]

        def at(p):
            return (s,) + p + (full, qcols(q))

        def final(p):
            return (tile[s],) + p + (full, qcols(q))
        dst_at = final if ph == 2 else at
        send_phase(core, coords, dim, lambda p: src.at[at(p)], lambda p: dst.at[dst_at(p)], tssem.at[ph], trsem.at[s, q, ph])
        keep_own(coords, dim, src, at, dst, dst_at)

    def tarrived(s, q, ph):
        wait_bytes(r1b.at[s, pl.ds(0, 3), full, full, full, qcols(q)], trsem.at[s, q, ph])

    for s in range(NG):
        for t in range(NT):
            arrived(1, s, t, 2)
        for q in range(NQ):
            acc = lax.dot_general(aa[s].reshape(CH * TR, N), bb[q].reshape(KQ, N), (((1,), (1,)), ((), ())),
                                  preferred_element_type=F32)
            sb[s, :, :, :, :, qcols(q)] = acc.astype(BF).reshape(SIDE, SIDE, SIDE, TR, KQ)
            if s == 0 and q == 0:
                pl.semaphore_wait(credit, GREETED)
            tphase(s, q, 0)
    for ph in (1, 2):
        for q in range(NQ):
            for s in range(NG):
                tarrived(s, q, ph - 1)
                tphase(s, q, ph)

    def swap(q):
        return pltpu.make_async_remote_copy(
            src_ref=sa.at[pl.ds(1 - core, 2), :, :, :, :, qcols(q)], dst_ref=r1a.at[pl.ds(0, 2), :, :, :, :, qcols(q)],
            send_sem=dssem.at[q], recv_sem=drsem.at[q], device_id=partner, device_id_type=MESH)

    def store(q):
        return pltpu.make_async_copy(obuf.at[q % 2], out_hbm.at[:, qcols(q), :], osem.at[q])

    def finish(q):
        def own(i):
            return sa[pl.ds(core, 2), i // SIDE, i % SIDE, :, :, qcols(q)].astype(F32)

        def par(i):
            return r1a[pl.ds(0, 2), i // SIDE, i % SIDE, :, :, qcols(q)].astype(F32)

        def add(i, acc):
            return acc + jnp.sum(own(i), axis=1) + jnp.sum(par(i), axis=1)
        zero = jnp.zeros((2, TR, KQ), F32)
        mean = lax.fori_loop(0, SIDE * SIDE, add, zero) * (1.0 / C)

        def add_sq(i, acc):
            u, v = own(i) - mean[:, None], par(i) - mean[:, None]
            return acc + jnp.sum(u * u, axis=1) + jnp.sum(v * v, axis=1)
        var = lax.fori_loop(0, SIDE * SIDE, add_sq, zero) * (1.0 / C)
        rstd = lax.rsqrt(var + LN_EPS)

        def spread(i, carry):
            for first, vals in ((core * CH, own(i)), ((1 - core) * CH, par(i))):
                for k in range(SIDE):
                    c = first + i * SIDE + k
                    v = (vals[:, k] - mean) * rstd * hid_ref[0, c] + hid_ref[1, c]
                    for b in range(2):
                        for lt in range(KQ // 128):
                            y[lt, pl.ds(b * TR * YSK + c, TR, stride=YSK), :] = v[b, :, lt * 128:(lt + 1) * 128]
            return carry
        lax.fori_loop(0, SIDE * SIDE, spread, 0)

        def row(r, carry):
            at = pl.ds((r + 4 * core) * YSK, C)
            yt = jnp.concatenate([y[lt, at, :] for lt in range(KQ // 128)], axis=1).astype(BF)
            update = lax.dot_general(yt, wo_ref[...], (((0,), (0,)), ((), ())), preferred_element_type=F32)
            gate = sigmoid(jnp.dot(xall[core * RL + r, qcols(q), :], wg_ref[...], preferred_element_type=F32))
            obuf[q % 2, r] = (zbuf[r, qcols(q), :].astype(F32) + gate * update).astype(BF)
            return carry
        lax.fori_loop(0, RL, row, 0, unroll=2)

    def ready(q):
        for s in range(NG):
            tarrived(s, q, 2)
        swap(q).start()

    ready(0)
    for q in range(NQ):
        if q + 1 < NQ:
            ready(q + 1)
        swap(q).wait_recv()
        if q >= 2:
            store(q - 2).wait()
        finish(q)
        store(q).start()
    for q in range(NQ):
        swap(q).wait_send()
    for ph in range(3):
        wait_bytes(r1a.at[:, pl.ds(0, 3)], tssem.at[ph])
    wait_bytes(r1a.at[:, pl.ds(0, 3)], ssem.at[1, 2])
    store(NQ - 2).wait()
    store(NQ - 1).wait()


def solution(mesh):
    row_spec = P(('data', 'dap'), None, None)
    mask_spec = P(('data', 'dap'), None)
    replicated = P()
    vspec = pl.BlockSpec(memory_space=VMEM)
    aspec = pl.BlockSpec(memory_space=ANY)

    def local_fn(z_loc, mask_loc, ln_scale, ln_bias, w_a, w_a_gate, w_b, w_b_gate, w_gate, ln_hid_scale, ln_hid_bias, w_out):
        sets = VMEM((NG, SIDE, SIDE, SIDE, TR, N), BF)
        hid = jnp.stack([ln_hid_scale, ln_hid_bias]).astype(F32)
        return pl.pallas_call(
            update_kernel, name='update',
            out_shape=jax.ShapeDtypeStruct((RL, N, C), BF),
            in_specs=[pl.BlockSpec(memory_space=pltpu.SMEM), aspec] + [vspec] * 9, out_specs=aspec,
            scratch_shapes=[
                VMEM((RL, N, C), BF), VMEM((2 * RL, N, C), BF), VMEM((2, RL, N), jnp.int32), VMEM((4, C, C), BF),
                VMEM((KT // 128, CH * SKEW, 128), F32), VMEM((KT // 128, CH * SKEW, 128), F32),
                sets, sets, sets, sets, sets, sets, sets, VMEM((SIDE, SIDE, SIDE, NG, TR, N), BF),
                VMEM((KQ // 128, 2 * TR * YSK, 128), F32), VMEM((2, RL, KQ, C), BF),
                DMA((NT + 1,)), DMA, DMA((NT,)), DMA((NT,)), DMA, DMA, DMA((2, 3)), DMA((2, NG, NT, 3)),
                DMA((3,)), DMA((NG, NQ, 3)), DMA((NQ,)), DMA((NQ,)), DMA((NQ,)), pltpu.SemaphoreType.REGULAR],
            compiler_params=pltpu.CompilerParams(collective_id=1, has_side_effects=True, vmem_limit_bytes=67043328),
        )(hid, z_loc, mask_loc, ln_scale.reshape(1, C), ln_bias.reshape(1, C), w_a, w_a_gate, w_b, w_b_gate, w_gate, w_out)

    return jax.shard_map(local_fn, mesh=mesh, in_specs=(row_spec, mask_spec) + (replicated,) * 10, out_specs=row_spec, check_vma=False)
```

```python
import functools

import jax
import jax.numpy as jnp
from jax import lax
from jax.experimental import pallas as pl
from jax.experimental.pallas import tpu as pltpu
from jax.sharding import PartitionSpec as P

LN_EPS = 1e-5
MESH = pl.DeviceIdType.MESH
DMA = pltpu.SemaphoreType.DMA
VMEM = pltpu.VMEM
ANY = pl.ANY
N = 1536
C = 128
SIDE = 4
CH = 64
RL = 12
TR = 8
NG = 3
KC = 256
PARTS = ((0, 256), (2, 512), (1, 512))
UNITS = [(s, at, width) for s, width in PARTS for at in range(0, N, width)]
KT = 512
NQ = 6
KQ = N // NQ
SKEW = 9
YSK = 129
BF = jnp.bfloat16
F32 = jnp.float32


def place():
    me = lax.axis_index('dap')
    chip, core = me // 2, me % 2
    return core, (chip // 16, (chip // 4) % 4, chip % 4)


def dev(coords, core):
    return {'dap': (coords[0] * 16 + coords[1] * 4 + coords[2]) * 2 + core}


def shift(coords, dim, by):
    return tuple((v + by) % SIDE if i == dim else v for i, v in enumerate(coords))


def pick(dim, at):
    return tuple(at if i == dim else slice(None) for i in range(3))


def greet(sem, core, coords):
    for dim in range(3):
        for by in range(1, SIDE):
            pl.semaphore_signal(sem, inc=1, device_id=dev(shift(coords, dim, by), core), device_id_type=MESH)
    pl.semaphore_signal(sem, inc=1, device_id=dev(coords, 1 - core), device_id_type=MESH)


GREETED = 3 * (SIDE - 1) + 1


def wait_bytes(ref, sem):
    pltpu.make_async_copy(ref, ref, sem).wait()


def send_phase(ring, coords, dim, src_at, dst_at, ssem, rsem):
    for to, device in ring[dim]:
        pltpu.make_async_remote_copy(
            src_ref=src_at(pick(dim, to)), dst_ref=dst_at(pick(dim, coords[dim])), send_sem=ssem, recv_sem=rsem,
            device_id=device, device_id_type=MESH).start()


def loop(steps, body, unroll=None):
    def step(i, carry):
        body(i)
        return carry
    lax.fori_loop(0, steps, step, 0, unroll=unroll)


def keep_own(coords, dim, src, src_at, dst, dst_at):
    own = pick(dim, coords[dim])
    dst[dst_at(own)] = src[src_at(own)]


def sigmoid(v):
    return 0.5 * jnp.tanh(0.5 * v) + 0.5


def update_kernel(z_hbm, mask_ref, scale_ref, bias_ref, wa_ref, wag_ref, wb_ref, wbg_ref, wg_ref, wo_ref, hs_ref, hb_ref, out_hbm,
                  zbuf, xall, mall, wt, stage_a, stage_b, sa, sb, r1a, r1b, r2a, r2b, aa, bb, y, obuf, hid,
                  zsem, xssem, xown, xmix, mrsem, msem, ssem, rsem, tssem, trsem, dssem, drsem, osem, credit):
    core, coords = place()
    barrier = pltpu.get_barrier_semaphore()
    greet(barrier, core, coords)
    partner = dev(coords, 1 - core)
    ring = [[((coords[d] + by) % SIDE, dev(shift(coords, d, by), core)) for by in (1, 3, 2)] for d in range(3)]
    own0, mix0 = 4 * core, 8 - 8 * core
    tile = [s + core * (2 - 2 * s) for s in range(NG)]
    full = slice(None)

    def qcols(q):
        return pl.ds(q * KQ, KQ)

    first = [u for u in UNITS if u[0] == 0]
    loads = [pltpu.make_async_copy(z_hbm.at[pl.ds(own0, TR), pl.ds(at, w)], zbuf.at[pl.ds(own0, TR), pl.ds(at, w)], zsem.at[n])
             for n, (_, at, w) in enumerate(first)]
    loads.append(pltpu.make_async_copy(z_hbm.at[pl.ds(mix0, 4)], zbuf.at[pl.ds(mix0, 4)], zsem.at[len(first)]))
    for cp in loads:
        cp.start()
    for i, w in enumerate((wa_ref, wag_ref, wb_ref, wbg_ref)):
        wt[i] = w[...].astype(F32).T.astype(BF)
    mall[core] = mask_ref[...]
    for i, h in enumerate((hs_ref, hb_ref)):
        hid[i] = jnp.broadcast_to(h[...].astype(F32), (C, C)).T
    scale = scale_ref[...].astype(F32)
    bias = bias_ref[...].astype(F32)
    half = pl.ds(pl.multiple_of(core * CH, CH), CH)
    wcat = jnp.concatenate([wt[i, half, :] for i in range(4)], axis=0)

    def norm(row0, rows, start, width):
        def body(i, carry):
            r = row0 + i
            for k in range(width // KC):
                at = pl.ds(start + k * KC, KC)
                v = zbuf[r, at, :].astype(F32)
                centered = v - jnp.mean(v, axis=-1, keepdims=True)
                var = jnp.mean(centered * centered, axis=-1, keepdims=True)
                xall[core * RL + r, at, :] = (centered * lax.rsqrt(var + LN_EPS) * scale + bias).astype(BF)
            return carry
        lax.fori_loop(0, rows, body, 0, unroll=2)

    def give_x(row0, rows, start, width, sem):
        block = xall.at[pl.ds(core * RL + row0, rows), pl.ds(start, width)]
        pltpu.make_async_remote_copy(src_ref=block, dst_ref=block, send_sem=xssem, recv_sem=sem,
                                     device_id=partner, device_id_type=MESH).start()

    bufs = ((sb, r1b, r2b), (sa, r1a, r2a))

    def phase(arr, n, ph):
        s, start, width = UNITS[n]
        cols = pl.ds(start, width)
        dim = (n + ph) % 3
        src = bufs[arr][ph]

        def at(p):
            return (s,) + p + (full, cols)

        def final(p):
            return p + (tile[s], full, cols) if arr == 0 else at(p)
        dst = (bb, aa)[arr] if ph == 2 else bufs[arr][ph + 1]
        dst_at = final if ph == 2 else at
        send_phase(ring, coords, dim, lambda p: src.at[at(p)], lambda p: dst.at[dst_at(p)], ssem.at[arr, ph],
                   rsem.at[arr, n, ph])
        keep_own(coords, dim, src, at, dst, dst_at)

    def arrived(arr, n, ph):
        s, start, width = UNITS[n]
        wait_bytes(r1a.at[s, pl.ds(0, 3), full, full, full, pl.ds(start, width)], rsem.at[arr, n, ph])

    def make_unit(n):
        s, start, width = UNITS[n]

        def project_row(i, carry):
            row = tile[s] * TR + i
            owner, within = row // RL, row % RL
            for j in range(width // KC):
                at = pl.ds(start + j * KC, KC)
                p = lax.dot_general(wcat, xall[row, at, :], (((1,), (1,)), ((), ())), preferred_element_type=F32)
                keep = mall[owner, pl.ds(within, 1), at].astype(F32)
                a = sigmoid(p[CH:2 * CH]) * p[:CH] * keep
                b = sigmoid(p[3 * CH:]) * p[2 * CH:3 * CH] * keep
                for u in range(KC // 128):
                    lanes = slice(u * 128, (u + 1) * 128)
                    kt = j * (KC // 128) + u
                    stage_a[kt, pl.ds(i, CH, stride=SKEW), :] = a[:, lanes]
                    stage_b[kt, pl.ds(i, CH, stride=SKEW), :] = b[:, lanes]
            return carry
        lax.fori_loop(0, TR, project_row, 0, unroll=4)
        for arr, stage in ((0, stage_b), (1, stage_a)):
            s_ref = bufs[arr][0]

            def pack(i):
                def pack_y(k):
                    def pack_x(m):
                        c = (i * SIDE + k) * SIDE + m
                        for j in range(width // KC):
                            v = jnp.concatenate([stage[2 * j + u, pl.ds(c * SKEW, TR), :] for u in range(2)], axis=1)
                            s_ref[s, i, k, m, :, pl.ds(start + j * KC, KC)] = v.astype(BF)
                    loop(SIDE, pack_x, unroll=SIDE)
                loop(SIDE, pack_y)
            loop(SIDE, pack)
            phase(arr, n, 0)

    def forward(arr, n, ph):
        arrived(arr, n, ph - 1)
        phase(arr, n, ph)

    for n, (s, start, width) in enumerate(UNITS):
        if s == 0:
            loads[n].wait()
            norm(own0, TR, start, width)
            if n == 0:
                pl.semaphore_wait(barrier, GREETED)
                mcopy = pltpu.make_async_remote_copy(src_ref=mask_ref, dst_ref=mall.at[core], send_sem=msem, recv_sem=mrsem,
                                                     device_id=partner, device_id_type=MESH)
                mcopy.start()
            give_x(own0, TR, start, width, xown.at[n])
        if n == len(first):
            mcopy.wait()
            for k, (_, at, w) in enumerate(first):
                wait_bytes(xall.at[pl.ds(0, TR), pl.ds(at, w)], xown.at[k])
        if n == len(first) + 1:
            loads[len(first)].wait()
            norm(mix0, 4, 0, N)
            give_x(mix0, 4, 0, N, xmix)
        if s == 1 and start == 0:
            wait_bytes(xall.at[pl.ds(0, 4)], xmix)
        make_unit(n)

    for n in range(len(UNITS)):
        forward(0, n, 1)
        forward(1, n, 1)
    for arr in range(2):
        for n in range(len(UNITS)):
            forward(arr, n, 2)
    for arr, ph in ((0, 0), (1, 0), (0, 1), (1, 1), (0, 2)):
        wait_bytes(r1a.at[:, pl.ds(0, 3)], ssem.at[arr, ph])
    greet(credit, core, coords)
    wait_bytes(zbuf, xssem)
    for n in range(len(UNITS)):
        arrived(0, n, 2)

    def tphase(s, q, ph):
        dim = (s + q + ph) % 3
        src = (sb, r1b, r2b)[ph]
        dst = (r1b, r2b, sa)[ph]

        def at(p):
            return (s,) + p + (full, qcols(q))

        def final(p):
            return (tile[s],) + p + (full, qcols(q))
        dst_at = final if ph == 2 else at
        send_phase(ring, coords, dim, lambda p: src.at[at(p)], lambda p: dst.at[dst_at(p)], tssem.at[ph], trsem.at[s, q, ph])
        keep_own(coords, dim, src, at, dst, dst_at)

    def tarrived(s, q, ph):
        wait_bytes(r1b.at[s, pl.ds(0, 3), full, full, full, qcols(q)], trsem.at[s, q, ph])

    order = [s for s, _ in PARTS]
    slab = N // SIDE
    for s in order:
        for n, unit in enumerate(UNITS):
            if unit[0] == s:
                arrived(1, n, 2)
        for k in range(SIDE):
            acc = lax.dot_general(aa[s].reshape(CH * TR, N), bb[k].reshape(slab, N), (((1,), (1,)), ((), ())),
                                  preferred_element_type=F32)
            sb[s, :, :, :, :, pl.ds(k * slab, slab)] = acc.astype(BF).reshape(SIDE, SIDE, SIDE, TR, slab)
            if s == order[0] and k == 0:
                pl.semaphore_wait(credit, GREETED)
            for q in range(NQ):
                if k * slab < (q + 1) * KQ <= (k + 1) * slab:
                    tphase(s, q, 0)
    for ph in (1, 2):
        for q in range(NQ):
            for s in order:
                tarrived(s, q, ph - 1)
                tphase(s, q, ph)

    def swap(q):
        return pltpu.make_async_remote_copy(
            src_ref=sa.at[pl.ds(1 - core, 2), :, :, :, :, qcols(q)], dst_ref=r1a.at[pl.ds(0, 2), :, :, :, :, qcols(q)],
            send_sem=dssem.at[q], recv_sem=drsem.at[q], device_id=partner, device_id_type=MESH)

    def store(q):
        return pltpu.make_async_copy(obuf.at[q % 2], out_hbm.at[:, qcols(q), :], osem.at[q])

    def finish(q):
        def own(i):
            return sa[pl.ds(core, 2), i // SIDE, i % SIDE, :, :, qcols(q)].astype(F32)

        def par(i):
            return r1a[pl.ds(0, 2), i // SIDE, i % SIDE, :, :, qcols(q)].astype(F32)

        def add(i, acc):
            return acc + jnp.sum(own(i), axis=1) + jnp.sum(par(i), axis=1)
        zero = jnp.zeros((2, TR, KQ), F32)
        mean = lax.fori_loop(0, SIDE * SIDE, add, zero) * (1.0 / C)

        def add_sq(i, acc):
            u, v = own(i) - mean[:, None], par(i) - mean[:, None]
            return acc + jnp.sum(u * u, axis=1) + jnp.sum(v * v, axis=1)
        var = lax.fori_loop(0, SIDE * SIDE, add_sq, zero) * (1.0 / C)
        rstd = lax.rsqrt(var + LN_EPS)

        def spread(i, carry):
            for first, vals in ((core * CH, own(i)), ((1 - core) * CH, par(i))):
                for k in range(SIDE):
                    c = first + i * SIDE + k
                    v = (vals[:, k] - mean) * rstd
                    for b in range(2):
                        for lt in range(KQ // 128):
                            y[lt, pl.ds(b * TR * YSK + c, TR, stride=YSK), :] = v[b, :, lt * 128:(lt + 1) * 128]
            return carry
        lax.fori_loop(0, SIDE * SIDE, spread, 0)
        if q + 1 < NQ:
            ready(q + 1)

        def row(r, carry):
            at = pl.ds((r + 4 * core) * YSK, C)
            yt = jnp.concatenate([y[lt, at, :] * hid[0] + hid[1] for lt in range(KQ // 128)], axis=1).astype(BF)
            update = lax.dot_general(yt, wo_ref[...], (((0,), (0,)), ((), ())), preferred_element_type=F32)
            gate = sigmoid(jnp.dot(xall[core * RL + r, qcols(q), :], wg_ref[...], preferred_element_type=F32))
            obuf[q % 2, r] = (zbuf[r, qcols(q), :].astype(F32) + gate * update).astype(BF)
            return carry
        lax.fori_loop(0, RL, row, 0, unroll=3)

    def ready(q):
        for s in range(NG):
            tarrived(s, q, 2)
        swap(q).start()

    ready(0)
    for q in range(NQ):
        swap(q).wait_recv()
        if q >= 2:
            store(q - 2).wait()
        finish(q)
        store(q).start()
    for q in range(NQ):
        swap(q).wait_send()
    for ph in range(3):
        wait_bytes(r1a.at[:, pl.ds(0, 3)], tssem.at[ph])
    wait_bytes(r1a.at[:, pl.ds(0, 3)], ssem.at[1, 2])
    store(NQ - 2).wait()
    store(NQ - 1).wait()


def solution(mesh):
    row_spec = P(('data', 'dap'), None, None)
    mask_spec = P(('data', 'dap'), None)
    replicated = P()
    vspec = pl.BlockSpec(memory_space=VMEM)
    aspec = pl.BlockSpec(memory_space=ANY)

    def local_fn(z_loc, mask_loc, ln_scale, ln_bias, w_a, w_a_gate, w_b, w_b_gate, w_gate, ln_hid_scale, ln_hid_bias, w_out):
        sets = VMEM((NG, SIDE, SIDE, SIDE, TR, N), BF)
        return pl.pallas_call(
            update_kernel, name='update',
            out_shape=jax.ShapeDtypeStruct((RL, N, C), BF),
            in_specs=[aspec] + [vspec] * 11, out_specs=aspec,
            scratch_shapes=[
                VMEM((RL, N, C), BF), VMEM((2 * RL, N, C), BF), VMEM((2, RL, N), jnp.int32), VMEM((4, C, C), BF),
                VMEM((KT // 128, CH * SKEW, 128), F32), VMEM((KT // 128, CH * SKEW, 128), F32),
                sets, sets, sets, sets, sets, sets, sets, VMEM((SIDE, SIDE, SIDE, NG, TR, N), BF),
                VMEM((KQ // 128, 2 * TR * YSK, 128), F32), VMEM((2, RL, KQ, C), BF), VMEM((2, C, C), F32),
                DMA((len(UNITS),)), DMA, DMA((len(UNITS),)), DMA, DMA, DMA, DMA((2, 3)), DMA((2, len(UNITS), 3)),
                DMA((3,)), DMA((NG, NQ, 3)), DMA((NQ,)), DMA((NQ,)), DMA((NQ,)), pltpu.SemaphoreType.REGULAR],
            compiler_params=pltpu.CompilerParams(collective_id=1, has_side_effects=True, vmem_limit_bytes=67043328),
        )(z_loc, mask_loc, ln_scale.reshape(1, C), ln_bias.reshape(1, C), w_a, w_a_gate, w_b, w_b_gate, w_gate, w_out,
          ln_hid_scale.reshape(1, C), ln_hid_bias.reshape(1, C))

    return jax.shard_map(local_fn, mesh=mesh, in_specs=(row_spec, mask_spec) + (replicated,) * 10, out_specs=row_spec, check_vma=False)
```

```python
import functools

import jax
import jax.numpy as jnp
from jax import lax
from jax.experimental import pallas as pl
from jax.experimental.pallas import tpu as pltpu
from jax.sharding import PartitionSpec as P

LN_EPS = 1e-5
MESH = pl.DeviceIdType.MESH
DMA = pltpu.SemaphoreType.DMA
VMEM = pltpu.VMEM
ANY = pl.ANY
N = 1536
C = 128
SIDE = 4
CH = 64
RL = 12
TR = 8
NG = 3
KC = 256
PARTS = ((0, 256), (2, 512), (1, 512))
UNITS = [(s, at, width) for s, width in PARTS for at in range(0, N, width)]
KT = 512
NQ = 6
KQ = N // NQ
SKEW = 9
YSK = 129
PASS = 4
BF = jnp.bfloat16
F32 = jnp.float32


def place():
    me = lax.axis_index('dap')
    chip, core = me // 2, me % 2
    return core, (chip // 16, (chip // 4) % 4, chip % 4)


def dev(coords, core):
    return {'dap': (coords[0] * 16 + coords[1] * 4 + coords[2]) * 2 + core}


def shift(coords, dim, by):
    return tuple((v + by) % SIDE if i == dim else v for i, v in enumerate(coords))


def pick(dim, at):
    return tuple(at if i == dim else slice(None) for i in range(3))


def greet(sem, core, coords):
    for dim in range(3):
        for by in range(1, SIDE):
            pl.semaphore_signal(sem, inc=1, device_id=dev(shift(coords, dim, by), core), device_id_type=MESH)
    pl.semaphore_signal(sem, inc=1, device_id=dev(coords, 1 - core), device_id_type=MESH)


GREETED = 3 * (SIDE - 1) + 1


def wait_bytes(ref, sem):
    pltpu.make_async_copy(ref, ref, sem).wait()


def send_phase(ring, coords, dim, src_at, dst_at, ssem, rsem):
    for to, device in ring[dim]:
        pltpu.make_async_remote_copy(
            src_ref=src_at(pick(dim, to)), dst_ref=dst_at(pick(dim, coords[dim])), send_sem=ssem, recv_sem=rsem,
            device_id=device, device_id_type=MESH).start()


def loop(steps, body, unroll=None):
    def step(i, carry):
        body(i)
        return carry
    lax.fori_loop(0, steps, step, 0, unroll=unroll)


def keep_own(coords, dim, src, src_at, dst, dst_at):
    own = pick(dim, coords[dim])
    dst[dst_at(own)] = src[src_at(own)]


def sigmoid(v):
    return 0.5 * jnp.tanh(0.5 * v) + 0.5


def hidden_norm(core, own, par, y, midway):
    def add(i, acc):
        return acc + jnp.sum(own(i), axis=1) + jnp.sum(par(i), axis=1)
    zero = jnp.zeros((2, TR, KQ), F32)
    mean = lax.fori_loop(0, SIDE * SIDE, add, zero) * (1.0 / C)

    def add_sq(i, acc):
        u, v = own(i) - mean[:, None], par(i) - mean[:, None]
        return acc + jnp.sum(u * u, axis=1) + jnp.sum(v * v, axis=1)
    var = lax.fori_loop(0, SIDE * SIDE, add_sq, zero) * (1.0 / C)
    rstd = lax.rsqrt(var + LN_EPS)
    midway()

    def spread(i):
        for first, vals in ((core * CH, own(i)), ((1 - core) * CH, par(i))):
            for k in range(SIDE):
                c = first + i * SIDE + k
                v = (vals[:, k] - mean) * rstd
                for b in range(2):
                    for lt in range(KQ // 128):
                        y[lt, pl.ds(b * TR * YSK + c, TR, stride=YSK), :] = v[b, :, lt * 128:(lt + 1) * 128]
    loop(SIDE * SIDE, spread)


def out_rows(core, y, hid, wo_ref, wg_ref, x_at, put, first=0, count=RL):
    def row(i):
        r = first + i
        at = pl.ds((r + 4 * core) * YSK, C)
        yt = jnp.concatenate([y[lt, at, :] * hid[0] + hid[1] for lt in range(KQ // 128)], axis=1).astype(BF)
        update = lax.dot_general(yt, wo_ref[...], (((0,), (0,)), ((), ())), preferred_element_type=F32)
        put(r, sigmoid(jnp.dot(x_at(r), wg_ref[...], preferred_element_type=F32)) * update)
    loop(count, row, unroll=3)


def set_hidden(hid, hs_ref, hb_ref):
    for i, h in enumerate((hs_ref, hb_ref)):
        hid[i] = jnp.broadcast_to(h[...].astype(F32), (C, C)).T


def last_kernel(part, own_hbm, par_hbm, x_hbm, z_hbm, wg_hbm, wo_hbm, hs_hbm, hb_hbm, out_hbm,
                keep, own_v, par_v, xv, zv, wg_ref, wo_ref, hs_ref, hb_ref, ov, y, hid, isem, ksem, osem):
    core = lax.axis_index('dap') % 2
    done = N - KQ
    cols = pl.ds(done, KQ)
    pairs = ((hs_hbm, hs_ref), (hb_hbm, hb_ref), (own_hbm, own_v), (par_hbm, par_v), (wg_hbm, wg_ref), (wo_hbm, wo_ref),
             (x_hbm, xv), (z_hbm.at[:, cols, :], zv))
    loads = [pltpu.make_async_copy(a, b, isem.at[n]) for n, (a, b) in enumerate(pairs)]
    some = [pl.ds(r, RL // PASS) for r in range(0, RL, RL // PASS)]
    ins = [pltpu.make_async_copy(part.at[r, pl.ds(0, done)], keep.at[r], ksem.at[n]) for n, r in enumerate(some)]
    outs = [pltpu.make_async_copy(keep.at[r], out_hbm.at[r, pl.ds(0, done)], osem.at[n]) for n, r in enumerate(some)]
    for cp in loads + ins:
        cp.start()
    for cp in loads[:4]:
        cp.wait()
    set_hidden(hid, hs_ref, hb_ref)

    def midway():
        for a, b in zip(ins, outs):
            a.wait()
            b.start()
        for cp in loads[4:]:
            cp.wait()

    def put(r, v):
        ov[r] = (zv[r].astype(F32) + v).astype(BF)
    hidden_norm(core, lambda i: own_v[:, i // SIDE, i % SIDE].astype(F32), lambda i: par_v[:, i // SIDE, i % SIDE].astype(F32), y, midway)
    ends = []
    for n in range(2):
        rows = pl.ds(n * RL // 2, RL // 2)
        out_rows(core, y, hid, wo_ref, wg_ref, lambda r: xv[r], put, n * RL // 2, RL // 2)
        ends.append(pltpu.make_async_copy(ov.at[rows], out_hbm.at[rows, cols, :], osem.at[PASS + n]))
        ends[-1].start()
    for cp in outs + ends:
        cp.wait()


def update_kernel(z_hbm, *refs):
    small, refs = refs[:11], refs[11:]
    (out_hbm, own_out, par_out, x_out, mask_ref, scale_ref, bias_ref, wa_ref, wag_ref, wb_ref, wbg_ref, wg_ref, wo_ref, hs_ref, hb_ref,
                  zbuf, xall, mall, wt, stage_a, stage_b, sa, sb, r1a, r1b, r2a, r2b, aa, bb, y, obuf, hid,
                  zsem, xssem, xown, xmix, mrsem, msem, ssem, rsem, lsem, dssem, drsem, osem, credit, wsem) = refs
    core, coords = place()
    barrier = pltpu.get_barrier_semaphore()
    greet(barrier, core, coords)
    partner = dev(coords, 1 - core)
    ring = [[((coords[d] + by) % SIDE, dev(shift(coords, d, by), core)) for by in (1, 3, 2)] for d in range(3)]
    own0, mix0 = 4 * core, 8 - 8 * core
    tile = [s + core * (2 - 2 * s) for s in range(NG)]
    full = slice(None)

    def qcols(q):
        return pl.ds(q * KQ, KQ)

    first = [u for u in UNITS if u[0] == 0]
    loads = [pltpu.make_async_copy(z_hbm.at[pl.ds(own0, TR), pl.ds(at, w)], zbuf.at[pl.ds(own0, TR), pl.ds(at, w)], zsem.at[n])
             for n, (_, at, w) in enumerate(first)]
    loads.append(pltpu.make_async_copy(z_hbm.at[pl.ds(mix0, 4)], zbuf.at[pl.ds(mix0, 4)], zsem.at[len(first)]))
    held = (mask_ref, scale_ref, bias_ref, wa_ref, wag_ref, wb_ref, wbg_ref, wg_ref, wo_ref, hs_ref, hb_ref)
    copies = [pltpu.make_async_copy(a, b, wsem.at[n]) for n, (a, b) in enumerate(zip(small, held))]
    loads[0].start()
    for cp in copies:
        cp.start()
    for cp in loads[1:]:
        cp.start()
    for cp in copies:
        cp.wait()
    for i, w in enumerate((wa_ref, wag_ref, wb_ref, wbg_ref)):
        wt[i] = w[...].astype(F32).T.astype(BF)
    mall[core] = mask_ref[...]
    set_hidden(hid, hs_ref, hb_ref)
    scale = scale_ref[...].astype(F32)
    bias = bias_ref[...].astype(F32)
    half = pl.ds(pl.multiple_of(core * CH, CH), CH)
    wcat = jnp.concatenate([wt[i, half, :] for i in range(4)], axis=0)

    average = jnp.full((C, C), 1.0 / C, BF)

    def norm(row0, rows, start, width):
        def body(i, carry):
            r = row0 + i
            for k in range(width // KC):
                at = pl.ds(start + k * KC, KC)
                v = zbuf[r, at, :]
                centered = v.astype(F32) - jnp.dot(v, average, preferred_element_type=F32)
                var = jnp.mean(centered * centered, axis=-1, keepdims=True)
                xall[core * RL + r, at, :] = (centered * lax.rsqrt(var + LN_EPS) * scale + bias).astype(BF)
            return carry
        lax.fori_loop(0, rows, body, 0, unroll=4 if width == KC else 1)

    def give_x(row0, rows, start, width, sem):
        block = xall.at[pl.ds(core * RL + row0, rows), pl.ds(start, width)]
        pltpu.make_async_remote_copy(src_ref=block, dst_ref=block, send_sem=xssem, recv_sem=sem,
                                     device_id=partner, device_id_type=MESH).start()

    bufs = ((sb, r1b, r2b), (sa, r1a, r2a))

    def unit_sem(arr, n, ph):
        if ph < 2:
            return rsem.at[arr, n, ph]
        return lsem.at[NG] if arr == 0 else lsem.at[UNITS[n][0]]

    def phase(arr, n, ph):
        s, start, width = UNITS[n]
        cols = pl.ds(start, width)
        dim = (n + ph) % 3
        src = bufs[arr][ph]

        def at(p):
            return (s,) + p + (full, cols)

        def final(p):
            return p + (tile[s], full, cols) if arr == 0 else at(p)
        dst = (bb, aa)[arr] if ph == 2 else bufs[arr][ph + 1]
        dst_at = final if ph == 2 else at
        send_phase(ring, coords, dim, lambda p: src.at[at(p)], lambda p: dst.at[dst_at(p)], ssem.at[arr, ph],
                   unit_sem(arr, n, ph))
        keep_own(coords, dim, src, at, dst, dst_at)

    def arrived(arr, n, ph):
        s, start, width = UNITS[n]
        wait_bytes(r1a.at[s, pl.ds(0, 3), full, full, full, pl.ds(start, width)], rsem.at[arr, n, ph])

    def make_unit(n):
        s, start, width = UNITS[n]

        def project_row(i, carry):
            row = tile[s] * TR + i
            owner, within = row // RL, row % RL
            for j in range(width // KC):
                at = pl.ds(start + j * KC, KC)
                p = lax.dot_general(wcat, xall[row, at, :], (((1,), (1,)), ((), ())), preferred_element_type=F32)
                keep = mall[owner, pl.ds(within, 1), at].astype(F32)
                a = sigmoid(p[CH:2 * CH]) * p[:CH] * keep
                b = sigmoid(p[3 * CH:]) * p[2 * CH:3 * CH] * keep
                for u in range(KC // 128):
                    lanes = slice(u * 128, (u + 1) * 128)
                    kt = j * (KC // 128) + u
                    stage_a[kt, pl.ds(i, CH, stride=SKEW), :] = a[:, lanes]
                    stage_b[kt, pl.ds(i, CH, stride=SKEW), :] = b[:, lanes]
            return carry
        lax.fori_loop(0, TR, project_row, 0, unroll=4)
        for arr, stage in ((0, stage_b), (1, stage_a)):
            s_ref = bufs[arr][0]

            def pack(i):
                def pack_y(k):
                    def pack_x(m):
                        c = (i * SIDE + k) * SIDE + m
                        for j in range(width // KC):
                            v = jnp.concatenate([stage[2 * j + u, pl.ds(c * SKEW, TR), :] for u in range(2)], axis=1)
                            s_ref[s, i, k, m, :, pl.ds(start + j * KC, KC)] = v.astype(BF)
                    loop(SIDE, pack_x, unroll=SIDE)
                loop(SIDE, pack_y)
            loop(SIDE, pack)
            phase(arr, n, 0)

    def forward(arr, n, ph):
        arrived(arr, n, ph - 1)
        phase(arr, n, ph)

    for n, (s, start, width) in enumerate(UNITS):
        if s == 0:
            loads[n].wait()
            norm(own0, TR, start, width)
            if n == 0:
                pl.semaphore_wait(barrier, GREETED)
                mcopy = pltpu.make_async_remote_copy(src_ref=mask_ref, dst_ref=mall.at[core], send_sem=msem, recv_sem=mrsem,
                                                     device_id=partner, device_id_type=MESH)
                mcopy.start()
            give_x(own0, TR, start, width, xown.at[n])
        if n == len(first):
            mcopy.wait()
            for k, (_, at, w) in enumerate(first):
                wait_bytes(xall.at[pl.ds(0, TR), pl.ds(at, w)], xown.at[k])
        if n == len(first) + 1:
            loads[len(first)].wait()
            norm(mix0, 4, 0, N)
            give_x(mix0, 4, 0, N, xmix)
        if s == 1 and start == 0:
            wait_bytes(xall.at[pl.ds(0, 4)], xmix)
        make_unit(n)

    for n in range(len(UNITS)):
        forward(0, n, 1)
        forward(1, n, 1)
    for arr in range(2):
        for n in range(len(UNITS)):
            forward(arr, n, 2)
    for arr, ph in ((0, 0), (1, 0), (0, 1), (1, 1), (0, 2)):
        wait_bytes(r1a.at[:, pl.ds(0, 3)], ssem.at[arr, ph])
    wait_bytes(r1a.at[:, pl.ds(0, 3)], lsem.at[NG])
    greet(credit, core, coords)
    wait_bytes(zbuf, xssem)

    x_copy = pltpu.make_async_copy(xall.at[pl.ds(core * RL, RL), qcols(NQ - 1)], x_out, msem)
    x_copy.start()

    def part_sem(s, q, ph):
        k = 2 * NG * NQ + q if ph == 2 else (s * NQ + q) * 2 + ph
        return rsem.at[k // (2 * len(UNITS)), (k // 2) % len(UNITS), k % 2]

    def tphase(s, q, ph):
        dim = (s + q + ph) % 3
        src = (sb, r1b, r2b)[ph]
        dst = (r1b, r2b, sa)[ph]

        def at(p):
            return (s,) + p + (full, qcols(q))

        def final(p):
            return (tile[s],) + p + (full, qcols(q))
        dst_at = final if ph == 2 else at
        send_phase(ring, coords, dim, lambda p: src.at[at(p)], lambda p: dst.at[dst_at(p)], ssem.at[0, ph], part_sem(s, q, ph))
        keep_own(coords, dim, src, at, dst, dst_at)

    def tarrived(s, q, ph):
        wait_bytes(r1b.at[s, pl.ds(0, 3), full, full, full, qcols(q)], part_sem(s, q, ph))

    order = [s for s, _ in PARTS]
    slab = N // SIDE
    for s in order:
        wait_bytes(r1a.at[s, pl.ds(0, 3)], lsem.at[s])
        for k in range(SIDE):
            acc = lax.dot_general(aa[s].reshape(CH * TR, N), bb[k].reshape(slab, N), (((1,), (1,)), ((), ())),
                                  preferred_element_type=F32)
            sb[s, :, :, :, :, pl.ds(k * slab, slab)] = acc.astype(BF).reshape(SIDE, SIDE, SIDE, TR, slab)
            if s == order[0] and k == 0:
                pl.semaphore_wait(credit, GREETED)
            for q in range(NQ):
                if k * slab < (q + 1) * KQ <= (k + 1) * slab:
                    tphase(s, q, 0)
    for ph in (1, 2):
        for q in range(NQ):
            for s in order:
                tarrived(s, q, ph - 1)
                tphase(s, q, ph)

    def swap(q):
        return pltpu.make_async_remote_copy(
            src_ref=sa.at[pl.ds(1 - core, 2), :, :, :, :, qcols(q)],
            dst_ref=r1a.at[pl.ds(0, 2), :, :, :, :, qcols(q)] if q < NQ - 1 else par_out,
            send_sem=dssem, recv_sem=drsem.at[q], device_id=partner, device_id_type=MESH)

    def store(q):
        return pltpu.make_async_copy(obuf.at[q % 2], out_hbm.at[:, qcols(q), :], osem.at[q])

    def finish(q):
        def own(i):
            return sa[pl.ds(core, 2), i // SIDE, i % SIDE, :, :, qcols(q)].astype(F32)

        def par(i):
            return r1a[pl.ds(0, 2), i // SIDE, i % SIDE, :, :, qcols(q)].astype(F32)

        def put(r, v):
            obuf[q % 2, r] = (zbuf[r, qcols(q), :].astype(F32) + v).astype(BF)
        hidden_norm(core, own, par, y, lambda: ready(q + 1))
        out_rows(core, y, hid, wo_ref, wg_ref, lambda r: xall[core * RL + r, qcols(q), :], put)

    def ready(q):
        wait_bytes(r1b.at[:, pl.ds(0, 3), full, full, full, qcols(q)], part_sem(0, q, 2))
        swap(q).start()
        if q == NQ - 1:
            own_copy.start()

    own_copy = pltpu.make_async_copy(sa.at[pl.ds(core, 2), :, :, :, :, qcols(NQ - 1)], own_out, osem.at[NQ - 1])
    ready(0)
    for q in range(NQ - 1):
        swap(q).wait_recv()
        if q >= 2:
            store(q - 2).wait()
        finish(q)
        store(q).start()
    wait_bytes(sa.at[pl.ds(0, 2)], dssem)
    for ph in range(3):
        wait_bytes(r1a.at[:, pl.ds(0, 3)], ssem.at[0, ph])
    wait_bytes(r1a.at[:, pl.ds(0, 3)], ssem.at[1, 2])
    x_copy.wait()
    store(NQ - 3).wait()
    store(NQ - 2).wait()
    own_copy.wait()
    swap(NQ - 1).wait_recv()


def solution(mesh):
    row_spec = P(('data', 'dap'), None, None)
    mask_spec = P(('data', 'dap'), None)
    replicated = P()
    aspec = pl.BlockSpec(memory_space=ANY)

    def local_fn(z_loc, mask_loc, ln_scale, ln_bias, w_a, w_a_gate, w_b, w_b_gate, w_gate, ln_hid_scale, ln_hid_bias, w_out):
        sets = VMEM((NG, SIDE, SIDE, SIDE, TR, N), BF)
        line, square = VMEM((1, C), BF), VMEM((C, C), BF)
        edge = jax.ShapeDtypeStruct((2, SIDE, SIDE, SIDE, TR, KQ), BF)
        hs, hb = ln_hid_scale.reshape(1, C), ln_hid_bias.reshape(1, C)
        part, own, par, x_last = pl.pallas_call(
            update_kernel, name='update',
            out_shape=(jax.ShapeDtypeStruct((RL, N, C), BF), edge, edge, jax.ShapeDtypeStruct((RL, KQ, C), BF)),
            in_specs=[aspec] * 12, out_specs=(aspec,) * 4,
            scratch_shapes=[VMEM((RL, N), jnp.int32), line, line] + [square] * 6 + [line] * 2 + [
                VMEM((RL, N, C), BF), VMEM((2 * RL, N, C), BF), VMEM((2, RL, N), jnp.int32), VMEM((4, C, C), BF),
                VMEM((KT // 128, CH * SKEW, 128), F32), VMEM((KT // 128, CH * SKEW, 128), F32),
                sets, sets, sets, sets, sets, sets, sets, VMEM((SIDE, SIDE, SIDE, NG, TR, N), BF),
                VMEM((KQ // 128, 2 * TR * YSK, 128), F32), VMEM((2, RL, KQ, C), BF), VMEM((2, C, C), F32),
                DMA((N // PARTS[0][1] + 1,)), DMA, DMA((N // PARTS[0][1],)), DMA, DMA, DMA, DMA((2, 3)), DMA((2, len(UNITS), 2)),
                DMA((NG + 1,)), DMA, DMA((NQ,)), DMA((NQ,)), pltpu.SemaphoreType.REGULAR, DMA((11,))],
            compiler_params=pltpu.CompilerParams(collective_id=1, has_side_effects=True, vmem_limit_bytes=67043328),
        )(z_loc, mask_loc, ln_scale.reshape(1, C), ln_bias.reshape(1, C), w_a, w_a_gate, w_b, w_b_gate, w_gate, w_out, hs, hb)
        edge_v = VMEM((2, SIDE, SIDE, SIDE, TR, KQ), BF)
        block = VMEM((RL, KQ, C), BF)
        return pl.pallas_call(
            last_kernel, name='last', out_shape=jax.ShapeDtypeStruct((RL, N, C), BF),
            in_specs=[aspec] * 9, out_specs=aspec,
            scratch_shapes=[VMEM((RL, N - KQ, C), BF), edge_v, edge_v, block, block, square, square, line, line, block,
                            VMEM((KQ // 128, 2 * TR * YSK, 128), F32), VMEM((2, C, C), F32), DMA((8,)), DMA((PASS,)), DMA((PASS + 2,))],
            compiler_params=pltpu.CompilerParams(vmem_limit_bytes=60 * 2**20),
        )(part, own, par, x_last, z_loc, w_gate, w_out, hs, hb)

    return jax.shard_map(local_fn, mesh=mesh, in_specs=(row_spec, mask_spec) + (replicated,) * 10, out_specs=row_spec, check_vma=False)
```

```python
import functools

import jax
import jax.numpy as jnp
from jax import lax
from jax.experimental import pallas as pl
from jax.experimental.pallas import tpu as pltpu
from jax.sharding import PartitionSpec as P

LN_EPS = 1e-5
MESH = pl.DeviceIdType.MESH
DMA = pltpu.SemaphoreType.DMA
VMEM = pltpu.VMEM
ANY = pl.ANY
N = 1536
C = 128
SIDE = 4
CH = 64
RL = 12
TR = 8
NG = 3
KC = 256
PARTS = ((0, 256), (2, 512), (1, 512))
UNITS = [(s, at, width) for s, width in PARTS for at in range(0, N, width)]
KT = 512
NQ = 6
KQ = N // NQ
SKEW = 9
YSK = 129
PASS = 4
BF = jnp.bfloat16
F32 = jnp.float32


def place():
    me = lax.axis_index('dap')
    chip, core = me // 2, me % 2
    return core, (chip // 16, (chip // 4) % 4, chip % 4)


def dev(coords, core):
    return {'dap': (coords[0] * 16 + coords[1] * 4 + coords[2]) * 2 + core}


def shift(coords, dim, by):
    return tuple((v + by) % SIDE if i == dim else v for i, v in enumerate(coords))


def pick(dim, at):
    return tuple(at if i == dim else slice(None) for i in range(3))


def greet(sem, core, coords):
    for dim in range(3):
        for by in range(1, SIDE):
            pl.semaphore_signal(sem, inc=1, device_id=dev(shift(coords, dim, by), core), device_id_type=MESH)
    pl.semaphore_signal(sem, inc=1, device_id=dev(coords, 1 - core), device_id_type=MESH)


GREETED = 3 * (SIDE - 1) + 1


def wait_bytes(ref, sem):
    pltpu.make_async_copy(ref, ref, sem).wait()


def send_phase(ring, coords, dim, src_at, dst_at, ssem, rsem):
    for to, device in ring[dim]:
        pltpu.make_async_remote_copy(
            src_ref=src_at(pick(dim, to)), dst_ref=dst_at(pick(dim, coords[dim])), send_sem=ssem, recv_sem=rsem,
            device_id=device, device_id_type=MESH).start()


def loop(steps, body, unroll=None):
    def step(i, carry):
        body(i)
        return carry
    lax.fori_loop(0, steps, step, 0, unroll=unroll)


def keep_own(coords, dim, src, src_at, dst, dst_at):
    own = pick(dim, coords[dim])
    dst[dst_at(own)] = src[src_at(own)]


def sigmoid(v):
    return 0.5 * jnp.tanh(0.5 * v) + 0.5


def hidden_norm(core, own, par, y, midway):
    def add(i, acc):
        return acc + jnp.sum(own(i), axis=1) + jnp.sum(par(i), axis=1)
    zero = jnp.zeros((2, TR, KQ), F32)
    mean = lax.fori_loop(0, SIDE * SIDE, add, zero, unroll=2) * (1.0 / C)

    def add_sq(i, acc):
        u, v = own(i) - mean[:, None], par(i) - mean[:, None]
        return acc + jnp.sum(u * u, axis=1) + jnp.sum(v * v, axis=1)
    var = lax.fori_loop(0, SIDE * SIDE, add_sq, zero, unroll=2) * (1.0 / C)
    rstd = lax.rsqrt(var + LN_EPS)
    midway()

    def spread(i):
        for first, vals in ((core * CH, own(i)), ((1 - core) * CH, par(i))):
            for k in range(SIDE):
                c = first + i * SIDE + k
                v = (vals[:, k] - mean) * rstd
                for b in range(2):
                    for lt in range(KQ // 128):
                        y[lt, pl.ds(b * TR * YSK + c, TR, stride=YSK), :] = v[b, :, lt * 128:(lt + 1) * 128]
    loop(SIDE * SIDE, spread, unroll=2)


def out_rows(core, y, hid, wo_ref, wg_ref, x_at, put, first=0, count=RL):
    def row(i):
        r = first + i
        at = pl.ds((r + 4 * core) * YSK, C)
        yt = jnp.concatenate([y[lt, at, :] * hid[0] + hid[1] for lt in range(KQ // 128)], axis=1).astype(BF)
        update = lax.dot_general(yt, wo_ref[...], (((0,), (0,)), ((), ())), preferred_element_type=F32)
        put(r, sigmoid(jnp.dot(x_at(r), wg_ref[...], preferred_element_type=F32)) * update)
    loop(count, row, unroll=6)


def set_hidden(hid, hs_ref, hb_ref):
    for i, h in enumerate((hs_ref, hb_ref)):
        hid[i] = jnp.broadcast_to(h[...].astype(F32), (C, C)).T


def last_kernel(part, own_hbm, par_hbm, x_hbm, z_hbm, wg_hbm, wo_hbm, hs_hbm, hb_hbm, out_hbm,
                keep, own_v, par_v, xv, zv, wg_ref, wo_ref, hs_ref, hb_ref, ov, y, hid, isem, ksem, osem):
    core = lax.axis_index('dap') % 2
    done = N - KQ
    cols = pl.ds(done, KQ)
    pairs = ((hs_hbm, hs_ref), (hb_hbm, hb_ref), (own_hbm, own_v), (par_hbm, par_v), (wg_hbm, wg_ref), (wo_hbm, wo_ref),
             (x_hbm, xv), (z_hbm.at[:, cols, :], zv))
    loads = [pltpu.make_async_copy(a, b, isem.at[n]) for n, (a, b) in enumerate(pairs)]
    some = [pl.ds(r, RL // PASS) for r in range(0, RL, RL // PASS)]
    ins = [pltpu.make_async_copy(part.at[r, pl.ds(0, done)], keep.at[r], ksem.at[n]) for n, r in enumerate(some)]
    outs = [pltpu.make_async_copy(keep.at[r], out_hbm.at[r, pl.ds(0, done)], osem.at[n]) for n, r in enumerate(some)]
    for cp in loads + ins:
        cp.start()
    for cp in loads[:4]:
        cp.wait()
    set_hidden(hid, hs_ref, hb_ref)

    def put(r, v):
        ov[r] = (zv[r].astype(F32) + v).astype(BF)
    hidden_norm(core, lambda i: own_v[:, i // SIDE, i % SIDE].astype(F32), lambda i: par_v[:, i // SIDE, i % SIDE].astype(F32), y, lambda: None)
    for cp in loads[4:]:
        cp.wait()
    ends = []
    for n in range(2):
        rows = pl.ds(n * RL // 2, RL // 2)
        out_rows(core, y, hid, wo_ref, wg_ref, lambda r: xv[r], put, n * RL // 2, RL // 2)
        ends.append(pltpu.make_async_copy(ov.at[rows], out_hbm.at[rows, cols, :], osem.at[PASS + n]))
        ends[-1].start()
        if n == 0:
            for a, b in zip(ins, outs):
                a.wait()
                b.start()
    for cp in outs + ends:
        cp.wait()


def update_kernel(z_hbm, *refs):
    small, refs = refs[:11], refs[11:]
    (out_hbm, own_out, par_out, x_out, mask_ref, scale_ref, bias_ref, wa_ref, wag_ref, wb_ref, wbg_ref, wg_ref, wo_ref, hs_ref, hb_ref,
                  zbuf, xall, mall, wt, stage_a, stage_b, sa, sb, r1a, r1b, r2a, r2b, aa, bb, y, obuf, hid,
                  zsem, xssem, xown, xmix, mrsem, msem, ssem, rsem, lsem, dssem, drsem, osem, credit, wsem) = refs
    core, coords = place()
    barrier = pltpu.get_barrier_semaphore()
    greet(barrier, core, coords)
    partner = dev(coords, 1 - core)
    ring = [[((coords[d] + by) % SIDE, dev(shift(coords, d, by), core)) for by in (1, 3, 2)] for d in range(3)]
    own0, mix0 = 4 * core, 8 - 8 * core
    tile = [s + core * (2 - 2 * s) for s in range(NG)]
    full = slice(None)

    def qcols(q):
        return pl.ds(q * KQ, KQ)

    first = [u for u in UNITS if u[0] == 0]
    loads = [pltpu.make_async_copy(z_hbm.at[pl.ds(own0, TR), pl.ds(at, w)], zbuf.at[pl.ds(own0, TR), pl.ds(at, w)], zsem.at[n])
             for n, (_, at, w) in enumerate(first)]
    loads.append(pltpu.make_async_copy(z_hbm.at[pl.ds(mix0, 4)], zbuf.at[pl.ds(mix0, 4)], zsem.at[len(first)]))
    held = (mask_ref, scale_ref, bias_ref, wa_ref, wag_ref, wb_ref, wbg_ref, wg_ref, wo_ref, hs_ref, hb_ref)
    copies = [pltpu.make_async_copy(a, b, wsem.at[n]) for n, (a, b) in enumerate(zip(small, held))]
    loads[0].start()
    for cp in copies:
        cp.start()
    for cp in copies:
        cp.wait()
    for cp in loads[1:]:
        cp.start()
    for i, w in enumerate((wa_ref, wag_ref, wb_ref, wbg_ref)):
        wt[i] = w[...].astype(F32).T.astype(BF)
    mall[core] = mask_ref[...]
    set_hidden(hid, hs_ref, hb_ref)
    scale = scale_ref[...].astype(F32)
    bias = bias_ref[...].astype(F32)
    half = pl.ds(pl.multiple_of(core * CH, CH), CH)
    wcat = jnp.concatenate([wt[i, half, :] for i in range(4)], axis=0)

    average = jnp.full((C, C), 1.0 / C, BF)

    def norm(row0, rows, start, width):
        def body(i, carry):
            r = row0 + i
            for k in range(width // KC):
                at = pl.ds(start + k * KC, KC)
                v = zbuf[r, at, :]
                centered = v.astype(F32) - jnp.dot(v, average, preferred_element_type=F32)
                var = jnp.mean(centered * centered, axis=-1, keepdims=True)
                xall[core * RL + r, at, :] = (centered * lax.rsqrt(var + LN_EPS) * scale + bias).astype(BF)
            return carry
        lax.fori_loop(0, rows, body, 0, unroll=4 if width == KC else 1)

    def give_x(row0, rows, start, width, sem):
        block = xall.at[pl.ds(core * RL + row0, rows), pl.ds(start, width)]
        pltpu.make_async_remote_copy(src_ref=block, dst_ref=block, send_sem=xssem, recv_sem=sem,
                                     device_id=partner, device_id_type=MESH).start()

    bufs = ((sb, r1b, r2b), (sa, r1a, r2a))

    def unit_sem(arr, n, ph):
        if ph < 2:
            return rsem.at[arr, n, ph]
        return lsem.at[NG] if arr == 0 else lsem.at[UNITS[n][0]]

    def phase(arr, n, ph):
        s, start, width = UNITS[n]
        cols = pl.ds(start, width)
        dim = (n + arr + ph) % 3
        src = bufs[arr][ph]

        def at(p):
            return (s,) + p + (full, cols)

        def final(p):
            return p + (tile[s], full, cols) if arr == 0 else at(p)
        dst = (bb, aa)[arr] if ph == 2 else bufs[arr][ph + 1]
        dst_at = final if ph == 2 else at
        send_phase(ring, coords, dim, lambda p: src.at[at(p)], lambda p: dst.at[dst_at(p)], ssem.at[arr, ph],
                   unit_sem(arr, n, ph))
        keep_own(coords, dim, src, at, dst, dst_at)

    def arrived(arr, n, ph):
        s, start, width = UNITS[n]
        wait_bytes(r1a.at[s, pl.ds(0, 3), full, full, full, pl.ds(start, width)], rsem.at[arr, n, ph])

    def make_unit(n):
        s, start, width = UNITS[n]

        def project_row(i, carry):
            row = tile[s] * TR + i
            owner, within = row // RL, row % RL
            for j in range(width // KC):
                at = pl.ds(start + j * KC, KC)
                p = lax.dot_general(wcat, xall[row, at, :], (((1,), (1,)), ((), ())), preferred_element_type=F32)
                keep = mall[owner, pl.ds(within, 1), at].astype(F32)
                a = sigmoid(p[CH:2 * CH]) * p[:CH] * keep
                b = sigmoid(p[3 * CH:]) * p[2 * CH:3 * CH] * keep
                for u in range(KC // 128):
                    lanes = slice(u * 128, (u + 1) * 128)
                    kt = j * (KC // 128) + u
                    stage_a[kt, pl.ds(i, CH, stride=SKEW), :] = a[:, lanes]
                    stage_b[kt, pl.ds(i, CH, stride=SKEW), :] = b[:, lanes]
            return carry
        lax.fori_loop(0, TR, project_row, 0, unroll=4)
        for arr, stage in ((0, stage_b), (1, stage_a)):
            s_ref = bufs[arr][0]

            def pack(i):
                def pack_y(k):
                    def pack_x(m):
                        c = (i * SIDE + k) * SIDE + m
                        for j in range(width // KC):
                            v = jnp.concatenate([stage[2 * j + u, pl.ds(c * SKEW, TR), :] for u in range(2)], axis=1)
                            s_ref[s, i, k, m, :, pl.ds(start + j * KC, KC)] = v.astype(BF)
                    loop(SIDE, pack_x, unroll=SIDE)
                loop(SIDE, pack_y)
            loop(SIDE, pack)
            phase(arr, n, 0)

    def forward(arr, n, ph):
        arrived(arr, n, ph - 1)
        phase(arr, n, ph)

    for n, (s, start, width) in enumerate(UNITS):
        if s == 0:
            loads[n].wait()
            norm(own0, TR, start, width)
            if n == 0:
                pl.semaphore_wait(barrier, GREETED)
                mcopy = pltpu.make_async_remote_copy(src_ref=mask_ref, dst_ref=mall.at[core], send_sem=msem, recv_sem=mrsem,
                                                     device_id=partner, device_id_type=MESH)
                mcopy.start()
            give_x(own0, TR, start, width, xown.at[n])
        if n == len(first):
            mcopy.wait()
            for k, (_, at, w) in enumerate(first):
                wait_bytes(xall.at[pl.ds(0, TR), pl.ds(at, w)], xown.at[k])
        if n == len(first) + 1:
            loads[len(first)].wait()
            norm(mix0, 4, 0, N)
            give_x(mix0, 4, 0, N, xmix)
        if s == 1 and start == 0:
            wait_bytes(xall.at[pl.ds(0, 4)], xmix)
        make_unit(n)

    for n in range(len(UNITS)):
        forward(0, n, 1)
        forward(1, n, 1)
    for arr in range(2):
        for n in range(len(UNITS)):
            forward(arr, n, 2)
    for arr, ph in ((0, 0), (1, 0), (0, 1), (1, 1), (0, 2)):
        wait_bytes(r1a.at[:, pl.ds(0, 3)], ssem.at[arr, ph])
    wait_bytes(r1a.at[:, pl.ds(0, 3)], lsem.at[NG])
    greet(credit, core, coords)
    wait_bytes(zbuf, xssem)

    x_copy = pltpu.make_async_copy(xall.at[pl.ds(core * RL, RL), qcols(NQ - 1)], x_out, msem)
    x_copy.start()

    def part_sem(s, q, ph):
        k = 2 * NG * NQ + q if ph == 2 else (s * NQ + q) * 2 + ph
        return rsem.at[k // (2 * len(UNITS)), (k // 2) % len(UNITS), k % 2]

    def tphase(s, q, ph):
        dim = (s + q + ph) % 3
        src = (sb, r1b, r2b)[ph]
        dst = (r1b, r2b, sa)[ph]

        def at(p):
            return (s,) + p + (full, qcols(q))

        def final(p):
            return (tile[s],) + p + (full, qcols(q))
        dst_at = final if ph == 2 else at
        send_phase(ring, coords, dim, lambda p: src.at[at(p)], lambda p: dst.at[dst_at(p)], ssem.at[0, ph], part_sem(s, q, ph))
        keep_own(coords, dim, src, at, dst, dst_at)

    def tarrived(s, q, ph):
        wait_bytes(r1b.at[s, pl.ds(0, 3), full, full, full, qcols(q)], part_sem(s, q, ph))

    order = [s for s, _ in PARTS]
    slab = N // SIDE
    for s in order:
        wait_bytes(r1a.at[s, pl.ds(0, 3)], lsem.at[s])
        for k in range(SIDE):
            acc = lax.dot_general(aa[s].reshape(CH * TR, N), bb[k].reshape(slab, N), (((1,), (1,)), ((), ())),
                                  preferred_element_type=F32)
            sb[s, :, :, :, :, pl.ds(k * slab, slab)] = acc.astype(BF).reshape(SIDE, SIDE, SIDE, TR, slab)
            if s == order[0] and k == 0:
                pl.semaphore_wait(credit, GREETED)
            for q in range(NQ):
                if k * slab < (q + 1) * KQ <= (k + 1) * slab:
                    tphase(s, q, 0)
    for ph in (1, 2):
        for q in range(NQ):
            for s in order:
                tarrived(s, q, ph - 1)
                tphase(s, q, ph)

    def swap(q):
        return pltpu.make_async_remote_copy(
            src_ref=sa.at[pl.ds(1 - core, 2), :, :, :, :, qcols(q)],
            dst_ref=r1a.at[pl.ds(0, 2), :, :, :, :, qcols(q)] if q < NQ - 1 else par_out,
            send_sem=dssem, recv_sem=drsem.at[q], device_id=partner, device_id_type=MESH)

    def store(q):
        return pltpu.make_async_copy(obuf.at[q % 2], out_hbm.at[:, qcols(q), :], osem.at[q])

    def finish(q):
        def own(i):
            return sa[pl.ds(core, 2), i // SIDE, i % SIDE, :, :, qcols(q)].astype(F32)

        def par(i):
            return r1a[pl.ds(0, 2), i // SIDE, i % SIDE, :, :, qcols(q)].astype(F32)

        def put(r, v):
            obuf[q % 2, r] = (zbuf[r, qcols(q), :].astype(F32) + v).astype(BF)
        hidden_norm(core, own, par, y, lambda: ready(q + 1))
        out_rows(core, y, hid, wo_ref, wg_ref, lambda r: xall[core * RL + r, qcols(q), :], put)

    def ready(q):
        wait_bytes(r1b.at[:, pl.ds(0, 3), full, full, full, qcols(q)], part_sem(0, q, 2))
        swap(q).start()
        if q == NQ - 1:
            own_copy.start()

    own_copy = pltpu.make_async_copy(sa.at[pl.ds(core, 2), :, :, :, :, qcols(NQ - 1)], own_out, osem.at[NQ - 1])
    ready(0)
    for q in range(NQ - 1):
        swap(q).wait_recv()
        if q >= 2:
            store(q - 2).wait()
        finish(q)
        store(q).start()
    wait_bytes(sa.at[pl.ds(0, 2)], dssem)
    for ph in range(3):
        wait_bytes(r1a.at[:, pl.ds(0, 3)], ssem.at[0, ph])
    wait_bytes(r1a.at[:, pl.ds(0, 3)], ssem.at[1, 2])
    x_copy.wait()
    store(NQ - 3).wait()
    store(NQ - 2).wait()
    own_copy.wait()
    swap(NQ - 1).wait_recv()


def solution(mesh):
    row_spec = P(('data', 'dap'), None, None)
    mask_spec = P(('data', 'dap'), None)
    replicated = P()
    aspec = pl.BlockSpec(memory_space=ANY)

    def local_fn(z_loc, mask_loc, ln_scale, ln_bias, w_a, w_a_gate, w_b, w_b_gate, w_gate, ln_hid_scale, ln_hid_bias, w_out):
        sets = VMEM((NG, SIDE, SIDE, SIDE, TR, N), BF)
        line, square = VMEM((1, C), BF), VMEM((C, C), BF)
        edge = jax.ShapeDtypeStruct((2, SIDE, SIDE, SIDE, TR, KQ), BF)
        hs, hb = ln_hid_scale.reshape(1, C), ln_hid_bias.reshape(1, C)
        part, own, par, x_last = pl.pallas_call(
            update_kernel, name='update',
            out_shape=(jax.ShapeDtypeStruct((RL, N, C), BF), edge, edge, jax.ShapeDtypeStruct((RL, KQ, C), BF)),
            in_specs=[aspec] * 12, out_specs=(aspec,) * 4,
            scratch_shapes=[VMEM((RL, N), jnp.int32), line, line] + [square] * 6 + [line] * 2 + [
                VMEM((RL, N, C), BF), VMEM((2 * RL, N, C), BF), VMEM((2, RL, N), jnp.int32), VMEM((4, C, C), BF),
                VMEM((KT // 128, CH * SKEW, 128), F32), VMEM((KT // 128, CH * SKEW, 128), F32),
                sets, sets, sets, sets, sets, sets, sets, VMEM((SIDE, SIDE, SIDE, NG, TR, N), BF),
                VMEM((KQ // 128, 2 * TR * YSK, 128), F32), VMEM((2, RL, KQ, C), BF), VMEM((2, C, C), F32),
                DMA((N // PARTS[0][1] + 1,)), DMA, DMA((N // PARTS[0][1],)), DMA, DMA, DMA, DMA((2, 3)), DMA((2, len(UNITS), 2)),
                DMA((NG + 1,)), DMA, DMA((NQ,)), DMA((NQ,)), pltpu.SemaphoreType.REGULAR, DMA((11,))],
            compiler_params=pltpu.CompilerParams(collective_id=1, has_side_effects=True, vmem_limit_bytes=67043328),
        )(z_loc, mask_loc, ln_scale.reshape(1, C), ln_bias.reshape(1, C), w_a, w_a_gate, w_b, w_b_gate, w_gate, w_out, hs, hb)
        edge_v = VMEM((2, SIDE, SIDE, SIDE, TR, KQ), BF)
        block = VMEM((RL, KQ, C), BF)
        return pl.pallas_call(
            last_kernel, name='last', out_shape=jax.ShapeDtypeStruct((RL, N, C), BF),
            in_specs=[aspec] * 9, out_specs=aspec,
            scratch_shapes=[VMEM((RL, N - KQ, C), BF), edge_v, edge_v, block, block, square, square, line, line, block,
                            VMEM((KQ // 128, 2 * TR * YSK, 128), F32), VMEM((2, C, C), F32), DMA((8,)), DMA((PASS,)), DMA((PASS + 2,))],
            compiler_params=pltpu.CompilerParams(vmem_limit_bytes=60 * 2**20),
        )(part, own, par, x_last, z_loc, w_gate, w_out, hs, hb)

    return jax.shard_map(local_fn, mesh=mesh, in_specs=(row_spec, mask_spec) + (replicated,) * 10, out_specs=row_spec, check_vma=False)
```

```python
import functools

import jax
import jax.numpy as jnp
from jax import lax
from jax.experimental import pallas as pl
from jax.experimental.pallas import tpu as pltpu
from jax.sharding import PartitionSpec as P

LN_EPS = 1e-5
MESH = pl.DeviceIdType.MESH
DMA = pltpu.SemaphoreType.DMA
VMEM = pltpu.VMEM
ANY = pl.ANY
N = 1536
C = 128
SIDE = 4
CH = 64
RL = 12
TR = 8
NG = 3
KC = 256
PARTS = ((0, 256), (2, 512), (1, 512))
UNITS = [(s, at, width) for s, width in PARTS for at in range(0, N, width)]
KT = 512
NQ = 6
KQ = N // NQ
SKEW = 9
YSK = 129
PASS = 4
BF = jnp.bfloat16
F32 = jnp.float32


def place():
    me = lax.axis_index('dap')
    chip, core = me // 2, me % 2
    return core, (chip // 16, (chip // 4) % 4, chip % 4)


def dev(coords, core):
    return {'dap': (coords[0] * 16 + coords[1] * 4 + coords[2]) * 2 + core}


def shift(coords, dim, by):
    return tuple((v + by) % SIDE if i == dim else v for i, v in enumerate(coords))


def pick(dim, at):
    return tuple(at if i == dim else slice(None) for i in range(3))


def greet(sem, core, coords):
    for dim in range(3):
        for by in range(1, SIDE):
            pl.semaphore_signal(sem, inc=1, device_id=dev(shift(coords, dim, by), core), device_id_type=MESH)
    pl.semaphore_signal(sem, inc=1, device_id=dev(coords, 1 - core), device_id_type=MESH)


GREETED = 3 * (SIDE - 1) + 1


def wait_bytes(ref, sem):
    pltpu.make_async_copy(ref, ref, sem).wait()


def send_phase(ring, coords, dim, src_at, dst_at, ssem, rsem):
    for to, device in ring[dim]:
        pltpu.make_async_remote_copy(
            src_ref=src_at(pick(dim, to)), dst_ref=dst_at(pick(dim, coords[dim])), send_sem=ssem, recv_sem=rsem,
            device_id=device, device_id_type=MESH).start()


def loop(steps, body, unroll=None):
    def step(i, carry):
        body(i)
        return carry
    lax.fori_loop(0, steps, step, 0, unroll=unroll)


def keep_own(coords, dim, src, src_at, dst, dst_at):
    own = pick(dim, coords[dim])
    dst[dst_at(own)] = src[src_at(own)]


def sigmoid(v):
    return 0.5 * jnp.tanh(0.5 * v) + 0.5


def hidden_norm(core, own, par, y, midway):
    def add(i, acc):
        return acc + jnp.sum(own(i), axis=1) + jnp.sum(par(i), axis=1)
    zero = jnp.zeros((2, TR, KQ), F32)
    mean = lax.fori_loop(0, SIDE * SIDE, add, zero, unroll=2) * (1.0 / C)

    def add_sq(i, acc):
        u, v = own(i) - mean[:, None], par(i) - mean[:, None]
        return acc + jnp.sum(u * u, axis=1) + jnp.sum(v * v, axis=1)
    var = lax.fori_loop(0, SIDE * SIDE, add_sq, zero, unroll=2) * (1.0 / C)
    rstd = lax.rsqrt(var + LN_EPS)
    midway()

    def spread(i):
        for first, vals in ((core * CH, own(i)), ((1 - core) * CH, par(i))):
            for k in range(SIDE):
                c = first + i * SIDE + k
                v = (vals[:, k] - mean) * rstd
                for b in range(2):
                    for lt in range(KQ // 128):
                        y[lt, pl.ds(b * TR * YSK + c, TR, stride=YSK), :] = v[b, :, lt * 128:(lt + 1) * 128]
    loop(SIDE * SIDE, spread, unroll=2)


def out_rows(core, y, hid, wo_ref, wg_ref, x_at, put, first=0, count=RL):
    def row(i):
        r = first + i
        at = pl.ds((r + 4 * core) * YSK, C)
        yt = jnp.concatenate([y[lt, at, :] * hid[0] + hid[1] for lt in range(KQ // 128)], axis=1).astype(BF)
        update = lax.dot_general(yt, wo_ref[...], (((0,), (0,)), ((), ())), preferred_element_type=F32)
        put(r, sigmoid(jnp.dot(x_at(r), wg_ref[...], preferred_element_type=F32)) * update)
    loop(count, row, unroll=6)


def set_hidden(hid, hs_ref, hb_ref):
    for i, h in enumerate((hs_ref, hb_ref)):
        hid[i] = jnp.broadcast_to(h[...].astype(F32), (C, C)).T


def last_kernel(part, own_hbm, par_hbm, x_hbm, z_hbm, wg_hbm, wo_hbm, hs_hbm, hb_hbm, out_hbm,
                keep, own_v, par_v, xv, zv, wg_ref, wo_ref, hs_ref, hb_ref, ov, y, hid, isem, ksem, osem):
    core = lax.axis_index('dap') % 2
    done = N - KQ
    cols = pl.ds(done, KQ)
    pairs = ((hs_hbm, hs_ref), (hb_hbm, hb_ref), (own_hbm, own_v), (par_hbm, par_v), (wg_hbm, wg_ref), (wo_hbm, wo_ref),
             (x_hbm, xv), (z_hbm.at[:, cols, :], zv))
    loads = [pltpu.make_async_copy(a, b, isem.at[n]) for n, (a, b) in enumerate(pairs)]
    some = [pl.ds(r, RL // PASS) for r in range(0, RL, RL // PASS)]
    ins = [pltpu.make_async_copy(part.at[r, pl.ds(0, done)], keep.at[r], ksem.at[n]) for n, r in enumerate(some)]
    outs = [pltpu.make_async_copy(keep.at[r], out_hbm.at[r, pl.ds(0, done)], osem.at[n]) for n, r in enumerate(some)]
    for cp in loads + ins:
        cp.start()
    for cp in loads[:4]:
        cp.wait()
    set_hidden(hid, hs_ref, hb_ref)

    def put(r, v):
        ov[r] = (zv[r].astype(F32) + v).astype(BF)
    hidden_norm(core, lambda i: own_v[:, i // SIDE, i % SIDE].astype(F32), lambda i: par_v[:, i // SIDE, i % SIDE].astype(F32), y, lambda: None)
    for a, b in zip(ins, outs):
        a.wait()
        b.start()
    for cp in loads[4:]:
        cp.wait()
    ends = []
    for n in range(2):
        rows = pl.ds(n * RL // 2, RL // 2)
        out_rows(core, y, hid, wo_ref, wg_ref, lambda r: xv[r], put, n * RL // 2, RL // 2)
        ends.append(pltpu.make_async_copy(ov.at[rows], out_hbm.at[rows, cols, :], osem.at[PASS + n]))
        ends[-1].start()
    for cp in outs + ends:
        cp.wait()


def update_kernel(z_hbm, *refs):
    small, refs = refs[:11], refs[11:]
    (out_hbm, own_out, par_out, x_out, mask_ref, scale_ref, bias_ref, wa_ref, wag_ref, wb_ref, wbg_ref, wg_ref, wo_ref, hs_ref, hb_ref,
                  zbuf, xall, mall, wt, stage_a, stage_b, sa, sb, r1a, r1b, r2a, r2b, aa, bb, y, obuf, hid,
                  zsem, xssem, xown, xmix, mrsem, msem, ssem, rsem, lsem, dssem, drsem, osem, credit, wsem) = refs
    core, coords = place()
    barrier = pltpu.get_barrier_semaphore()
    greet(barrier, core, coords)
    partner = dev(coords, 1 - core)
    ring = [[((coords[d] + by) % SIDE, dev(shift(coords, d, by), core)) for by in (1, 3, 2)] for d in range(3)]
    own0, mix0 = 4 * core, 8 - 8 * core
    tile = [s + core * (2 - 2 * s) for s in range(NG)]
    full = slice(None)

    def qcols(q):
        return pl.ds(q * KQ, KQ)

    first = [u for u in UNITS if u[0] == 0]
    loads = [pltpu.make_async_copy(z_hbm.at[pl.ds(own0, TR), pl.ds(at, w)], zbuf.at[pl.ds(own0, TR), pl.ds(at, w)], zsem.at[n])
             for n, (_, at, w) in enumerate(first)]
    loads.append(pltpu.make_async_copy(z_hbm.at[pl.ds(mix0, 4)], zbuf.at[pl.ds(mix0, 4)], zsem.at[len(first)]))
    held = (mask_ref, scale_ref, bias_ref, wa_ref, wag_ref, wb_ref, wbg_ref, wg_ref, wo_ref, hs_ref, hb_ref)
    copies = [pltpu.make_async_copy(a, b, wsem.at[n]) for n, (a, b) in enumerate(zip(small, held))]
    loads[0].start()
    for cp in copies:
        cp.start()
    for cp in copies:
        cp.wait()
    for cp in loads[1:]:
        cp.start()
    for i, w in enumerate((wa_ref, wag_ref, wb_ref, wbg_ref)):
        wt[i] = w[...].astype(F32).T.astype(BF)
    mall[core] = mask_ref[...]
    scale = scale_ref[...].astype(F32)
    bias = bias_ref[...].astype(F32)
    half = pl.ds(pl.multiple_of(core * CH, CH), CH)
    wcat = jnp.concatenate([wt[i, half, :] for i in range(4)], axis=0)

    average = jnp.full((C, C), 1.0 / C, BF)

    def norm(row0, rows, start, width):
        def body(i, carry):
            r = row0 + i
            for k in range(width // KC):
                at = pl.ds(start + k * KC, KC)
                v = zbuf[r, at, :]
                centered = v.astype(F32) - jnp.dot(v, average, preferred_element_type=F32)
                var = jnp.mean(centered * centered, axis=-1, keepdims=True)
                xall[core * RL + r, at, :] = (centered * lax.rsqrt(var + LN_EPS) * scale + bias).astype(BF)
            return carry
        lax.fori_loop(0, rows, body, 0, unroll=8 if width == KC else 1)

    def give_x(row0, rows, start, width, sem):
        block = xall.at[pl.ds(core * RL + row0, rows), pl.ds(start, width)]
        pltpu.make_async_remote_copy(src_ref=block, dst_ref=block, send_sem=xssem, recv_sem=sem,
                                     device_id=partner, device_id_type=MESH).start()

    bufs = ((sb, r1b, r2b), (sa, r1a, r2a))

    def unit_sem(arr, n, ph):
        if ph < 2:
            return rsem.at[arr, n, ph]
        return lsem.at[NG] if arr == 0 else lsem.at[UNITS[n][0]]

    def phase(arr, n, ph):
        s, start, width = UNITS[n]
        cols = pl.ds(start, width)
        dim = (n + arr + ph) % 3
        src = bufs[arr][ph]

        def at(p):
            return (s,) + p + (full, cols)

        def final(p):
            return p + (tile[s], full, cols) if arr == 0 else at(p)
        dst = (bb, aa)[arr] if ph == 2 else bufs[arr][ph + 1]
        dst_at = final if ph == 2 else at
        send_phase(ring, coords, dim, lambda p: src.at[at(p)], lambda p: dst.at[dst_at(p)], ssem.at[arr, ph],
                   unit_sem(arr, n, ph))
        keep_own(coords, dim, src, at, dst, dst_at)

    def arrived(arr, n, ph):
        s, start, width = UNITS[n]
        wait_bytes(r1a.at[s, pl.ds(0, 3), full, full, full, pl.ds(start, width)], rsem.at[arr, n, ph])

    def make_unit(n):
        s, start, width = UNITS[n]

        def project_row(i, carry):
            row = tile[s] * TR + i
            owner, within = row // RL, row % RL
            for j in range(width // KC):
                at = pl.ds(start + j * KC, KC)
                p = lax.dot_general(wcat, xall[row, at, :], (((1,), (1,)), ((), ())), preferred_element_type=F32)
                keep = mall[owner, pl.ds(within, 1), at].astype(F32)
                a = sigmoid(p[CH:2 * CH]) * p[:CH] * keep
                b = sigmoid(p[3 * CH:]) * p[2 * CH:3 * CH] * keep
                for u in range(KC // 128):
                    lanes = slice(u * 128, (u + 1) * 128)
                    kt = j * (KC // 128) + u
                    stage_a[kt, pl.ds(i, CH, stride=SKEW), :] = a[:, lanes]
                    stage_b[kt, pl.ds(i, CH, stride=SKEW), :] = b[:, lanes]
            return carry
        lax.fori_loop(0, TR, project_row, 0, unroll=8 if width == KC else 4)
        for arr, stage in ((0, stage_b), (1, stage_a)):
            s_ref = bufs[arr][0]

            def pack(i):
                def pack_y(k):
                    def pack_x(m):
                        c = (i * SIDE + k) * SIDE + m
                        for j in range(width // KC):
                            v = jnp.concatenate([stage[2 * j + u, pl.ds(c * SKEW, TR), :] for u in range(2)], axis=1)
                            s_ref[s, i, k, m, :, pl.ds(start + j * KC, KC)] = v.astype(BF)
                    loop(SIDE, pack_x, unroll=SIDE)
                loop(SIDE, pack_y)
            loop(SIDE, pack)
            phase(arr, n, 0)

    def forward(arr, n, ph):
        arrived(arr, n, ph - 1)
        phase(arr, n, ph)

    for n, (s, start, width) in enumerate(UNITS):
        if s == 0:
            loads[n].wait()
            norm(own0, TR, start, width)
            if n == 0:
                pl.semaphore_wait(barrier, GREETED)
                mcopy = pltpu.make_async_remote_copy(src_ref=mask_ref, dst_ref=mall.at[core], send_sem=msem, recv_sem=mrsem,
                                                     device_id=partner, device_id_type=MESH)
                mcopy.start()
            give_x(own0, TR, start, width, xown.at[n])
        if n == len(first):
            mcopy.wait()
            for k, (_, at, w) in enumerate(first):
                wait_bytes(xall.at[pl.ds(0, TR), pl.ds(at, w)], xown.at[k])
        if n == len(first) + 1:
            loads[len(first)].wait()
            norm(mix0, 4, 0, N)
            give_x(mix0, 4, 0, N, xmix)
        if s == 1 and start == 0:
            wait_bytes(xall.at[pl.ds(0, 4)], xmix)
        make_unit(n)

    for n in range(len(UNITS)):
        forward(0, n, 1)
        forward(1, n, 1)
    for arr in range(2):
        for n in range(len(UNITS)):
            forward(arr, n, 2)
    for arr, ph in ((0, 0), (1, 0), (0, 1), (1, 1), (0, 2)):
        wait_bytes(r1a.at[:, pl.ds(0, 3)], ssem.at[arr, ph])
    wait_bytes(r1a.at[:, pl.ds(0, 3)], lsem.at[NG])
    greet(credit, core, coords)
    wait_bytes(zbuf, xssem)

    x_copy = pltpu.make_async_copy(xall.at[pl.ds(core * RL, RL), qcols(NQ - 1)], x_out, msem)
    x_copy.start()
    set_hidden(hid, hs_ref, hb_ref)

    def part_sem(s, q, ph):
        k = 2 * NG * NQ + q if ph == 2 else (s * NQ + q) * 2 + ph
        return rsem.at[k // (2 * len(UNITS)), (k // 2) % len(UNITS), k % 2]

    def tphase(s, q, ph):
        dim = (s + q + ph) % 3
        src = (sb, r1b, r2b)[ph]
        dst = (r1b, r2b, sa)[ph]

        def at(p):
            return (s,) + p + (full, qcols(q))

        def final(p):
            return (tile[s],) + p + (full, qcols(q))
        dst_at = final if ph == 2 else at
        send_phase(ring, coords, dim, lambda p: src.at[at(p)], lambda p: dst.at[dst_at(p)], ssem.at[0, ph], part_sem(s, q, ph))
        keep_own(coords, dim, src, at, dst, dst_at)

    def tarrived(s, q, ph):
        wait_bytes(r1b.at[s, pl.ds(0, 3), full, full, full, qcols(q)], part_sem(s, q, ph))

    order = [s for s, _ in PARTS]
    slab = N // SIDE
    for s in order:
        wait_bytes(r1a.at[s, pl.ds(0, 3)], lsem.at[s])
        for k in range(SIDE):
            acc = lax.dot_general(aa[s].reshape(CH * TR, N), bb[k].reshape(slab, N), (((1,), (1,)), ((), ())),
                                  preferred_element_type=F32)
            sb[s, :, :, :, :, pl.ds(k * slab, slab)] = acc.astype(BF).reshape(SIDE, SIDE, SIDE, TR, slab)
            if s == order[0] and k == 0:
                pl.semaphore_wait(credit, GREETED)
            for q in range(NQ):
                if k * slab < (q + 1) * KQ <= (k + 1) * slab:
                    tphase(s, q, 0)
    for ph in (1, 2):
        for q in range(NQ):
            for s in order:
                tarrived(s, q, ph - 1)
                tphase(s, q, ph)

    def swap(q):
        return pltpu.make_async_remote_copy(
            src_ref=sa.at[pl.ds(1 - core, 2), :, :, :, :, qcols(q)],
            dst_ref=r1a.at[pl.ds(0, 2), :, :, :, :, qcols(q)] if q < NQ - 1 else par_out,
            send_sem=dssem, recv_sem=drsem.at[q], device_id=partner, device_id_type=MESH)

    def store(q):
        return pltpu.make_async_copy(obuf.at[q % 2], out_hbm.at[:, qcols(q), :], osem.at[q])

    def finish(q):
        def own(i):
            return sa[pl.ds(core, 2), i // SIDE, i % SIDE, :, :, qcols(q)].astype(F32)

        def par(i):
            return r1a[pl.ds(0, 2), i // SIDE, i % SIDE, :, :, qcols(q)].astype(F32)

        def put(r, v):
            obuf[q % 2, r] = (zbuf[r, qcols(q), :].astype(F32) + v).astype(BF)
        hidden_norm(core, own, par, y, lambda: ready(q + 1))
        out_rows(core, y, hid, wo_ref, wg_ref, lambda r: xall[core * RL + r, qcols(q), :], put)

    def ready(q):
        wait_bytes(r1b.at[:, pl.ds(0, 3), full, full, full, qcols(q)], part_sem(0, q, 2))
        swap(q).start()
        if q == NQ - 1:
            own_copy.start()

    own_copy = pltpu.make_async_copy(sa.at[pl.ds(core, 2), :, :, :, :, qcols(NQ - 1)], own_out, osem.at[NQ - 1])
    ready(0)
    for q in range(NQ - 1):
        swap(q).wait_recv()
        if q >= 2:
            store(q - 2).wait()
        finish(q)
        store(q).start()
    wait_bytes(sa.at[pl.ds(0, 2)], dssem)
    for ph in range(3):
        wait_bytes(r1a.at[:, pl.ds(0, 3)], ssem.at[0, ph])
    wait_bytes(r1a.at[:, pl.ds(0, 3)], ssem.at[1, 2])
    x_copy.wait()
    store(NQ - 3).wait()
    store(NQ - 2).wait()
    own_copy.wait()
    swap(NQ - 1).wait_recv()


def solution(mesh):
    row_spec = P(('data', 'dap'), None, None)
    mask_spec = P(('data', 'dap'), None)
    replicated = P()
    aspec = pl.BlockSpec(memory_space=ANY)

    def local_fn(z_loc, mask_loc, ln_scale, ln_bias, w_a, w_a_gate, w_b, w_b_gate, w_gate, ln_hid_scale, ln_hid_bias, w_out):
        sets = VMEM((NG, SIDE, SIDE, SIDE, TR, N), BF)
        line, square = VMEM((1, C), BF), VMEM((C, C), BF)
        edge = jax.ShapeDtypeStruct((2, SIDE, SIDE, SIDE, TR, KQ), BF)
        hs, hb = ln_hid_scale.reshape(1, C), ln_hid_bias.reshape(1, C)
        part, own, par, x_last = pl.pallas_call(
            update_kernel, name='update',
            out_shape=(jax.ShapeDtypeStruct((RL, N, C), BF), edge, edge, jax.ShapeDtypeStruct((RL, KQ, C), BF)),
            in_specs=[aspec] * 12, out_specs=(aspec,) * 4,
            scratch_shapes=[VMEM((RL, N), jnp.int32), line, line] + [square] * 6 + [line] * 2 + [
                VMEM((RL, N, C), BF), VMEM((2 * RL, N, C), BF), VMEM((2, RL, N), jnp.int32), VMEM((4, C, C), BF),
                VMEM((KT // 128, CH * SKEW, 128), F32), VMEM((KT // 128, CH * SKEW, 128), F32),
                sets, sets, sets, sets, sets, sets, sets, VMEM((SIDE, SIDE, SIDE, NG, TR, N), BF),
                VMEM((KQ // 128, 2 * TR * YSK, 128), F32), VMEM((2, RL, KQ, C), BF), VMEM((2, C, C), F32),
                DMA((N // PARTS[0][1] + 1,)), DMA, DMA((N // PARTS[0][1],)), DMA, DMA, DMA, DMA((2, 3)), DMA((2, len(UNITS), 2)),
                DMA((NG + 1,)), DMA, DMA((NQ,)), DMA((NQ,)), pltpu.SemaphoreType.REGULAR, DMA((11,))],
            compiler_params=pltpu.CompilerParams(collective_id=1, has_side_effects=True, vmem_limit_bytes=67043328),
        )(z_loc, mask_loc, ln_scale.reshape(1, C), ln_bias.reshape(1, C), w_a, w_a_gate, w_b, w_b_gate, w_gate, w_out, hs, hb)
        edge_v = VMEM((2, SIDE, SIDE, SIDE, TR, KQ), BF)
        block = VMEM((RL, KQ, C), BF)
        return pl.pallas_call(
            last_kernel, name='last', out_shape=jax.ShapeDtypeStruct((RL, N, C), BF),
            in_specs=[aspec] * 9, out_specs=aspec,
            scratch_shapes=[VMEM((RL, N - KQ, C), BF), edge_v, edge_v, block, block, square, square, line, line, block,
                            VMEM((KQ // 128, 2 * TR * YSK, 128), F32), VMEM((2, C, C), F32), DMA((8,)), DMA((PASS,)), DMA((PASS + 2,))],
            compiler_params=pltpu.CompilerParams(vmem_limit_bytes=60 * 2**20),
        )(part, own, par, x_last, z_loc, w_gate, w_out, hs, hb)

    return jax.shard_map(local_fn, mesh=mesh, in_specs=(row_spec, mask_spec) + (replicated,) * 10, out_specs=row_spec, check_vma=False)
```

```python
import functools

import jax
import jax.numpy as jnp
from jax import lax
from jax.experimental import pallas as pl
from jax.experimental.pallas import tpu as pltpu
from jax.sharding import PartitionSpec as P

LN_EPS = 1e-5
MESH = pl.DeviceIdType.MESH
DMA = pltpu.SemaphoreType.DMA
VMEM = pltpu.VMEM
ANY = pl.ANY
N = 1536
C = 128
SIDE = 4
CH = 64
RL = 12
TR = 8
NG = 3
KC = 256
PARTS = ((0, 256), (2, 512), (1, 512))
UNITS = [(s, at, width) for s, width in PARTS for at in range(0, N, width)]
KT = 512
NQ = 6
KQ = N // NQ
SKEW = 9
YSK = 129
PASS = 4
BF = jnp.bfloat16
F32 = jnp.float32


def place():
    me = lax.axis_index('dap')
    chip, core = me // 2, me % 2
    return core, (chip // 16, (chip // 4) % 4, chip % 4)


def dev(coords, core):
    return {'dap': (coords[0] * 16 + coords[1] * 4 + coords[2]) * 2 + core}


def shift(coords, dim, by):
    return tuple((v + by) % SIDE if i == dim else v for i, v in enumerate(coords))


def pick(dim, at):
    return tuple(at if i == dim else slice(None) for i in range(3))


def greet(sem, core, coords):
    for dim in range(3):
        for by in range(1, SIDE):
            pl.semaphore_signal(sem, inc=1, device_id=dev(shift(coords, dim, by), core), device_id_type=MESH)
    pl.semaphore_signal(sem, inc=1, device_id=dev(coords, 1 - core), device_id_type=MESH)


GREETED = 3 * (SIDE - 1) + 1


def wait_bytes(ref, sem):
    pltpu.make_async_copy(ref, ref, sem).wait()


def send_phase(ring, coords, dim, src_at, dst_at, ssem, rsem):
    for to, device in ring[dim]:
        pltpu.make_async_remote_copy(
            src_ref=src_at(pick(dim, to)), dst_ref=dst_at(pick(dim, coords[dim])), send_sem=ssem, recv_sem=rsem,
            device_id=device, device_id_type=MESH).start()


def loop(steps, body, unroll=None):
    def step(i, carry):
        body(i)
        return carry
    lax.fori_loop(0, steps, step, 0, unroll=unroll)


def keep_own(coords, dim, src, src_at, dst, dst_at):
    own = pick(dim, coords[dim])
    dst[dst_at(own)] = src[src_at(own)]


def sigmoid(v):
    return 0.5 * jnp.tanh(0.5 * v) + 0.5


def hidden_norm(core, own, par, y, midway):
    def add(i, acc):
        return acc + jnp.sum(own(i), axis=1) + jnp.sum(par(i), axis=1)
    zero = jnp.zeros((2, TR, KQ), F32)
    mean = lax.fori_loop(0, SIDE * SIDE, add, zero, unroll=2) * (1.0 / C)

    def add_sq(i, acc):
        u, v = own(i) - mean[:, None], par(i) - mean[:, None]
        return acc + jnp.sum(u * u, axis=1) + jnp.sum(v * v, axis=1)
    var = lax.fori_loop(0, SIDE * SIDE, add_sq, zero, unroll=2) * (1.0 / C)
    rstd = lax.rsqrt(var + LN_EPS)
    midway()

    def spread(i):
        for first, vals in ((core * CH, own(i)), ((1 - core) * CH, par(i))):
            for k in range(SIDE):
                c = first + i * SIDE + k
                v = (vals[:, k] - mean) * rstd
                for b in range(2):
                    for lt in range(KQ // 128):
                        y[lt, pl.ds(b * TR * YSK + c, TR, stride=YSK), :] = v[b, :, lt * 128:(lt + 1) * 128]
    loop(SIDE * SIDE, spread, unroll=2)


def out_rows(core, y, hid, wo_ref, wg_ref, x_at, put, first=0, count=RL):
    def row(i):
        r = first + i
        at = pl.ds((r + 4 * core) * YSK, C)
        yt = jnp.concatenate([y[lt, at, :] * hid[0] + hid[1] for lt in range(KQ // 128)], axis=1).astype(BF)
        update = lax.dot_general(yt, wo_ref[...], (((0,), (0,)), ((), ())), preferred_element_type=F32)
        put(r, sigmoid(jnp.dot(x_at(r), wg_ref[...], preferred_element_type=F32)) * update)
    loop(count, row, unroll=6)


def set_hidden(hid, hs_ref, hb_ref):
    for i, h in enumerate((hs_ref, hb_ref)):
        hid[i] = jnp.broadcast_to(h[...].astype(F32), (C, C)).T


def last_kernel(part, own_hbm, par_hbm, x_hbm, z_hbm, wg_hbm, wo_hbm, hs_hbm, hb_hbm, out_hbm,
                keep, own_v, par_v, xv, zv, wg_ref, wo_ref, hs_ref, hb_ref, ov, y, hid, isem, ksem, osem):
    core = lax.axis_index('dap') % 2
    done = N - KQ
    cols = pl.ds(done, KQ)
    pairs = ((hs_hbm, hs_ref), (hb_hbm, hb_ref), (own_hbm, own_v), (par_hbm, par_v), (wg_hbm, wg_ref), (wo_hbm, wo_ref),
             (x_hbm, xv), (z_hbm.at[:, cols, :], zv))
    loads = [pltpu.make_async_copy(a, b, isem.at[n]) for n, (a, b) in enumerate(pairs)]
    some = [pl.ds(r, RL // PASS) for r in range(0, RL, RL // PASS)]
    ins = [pltpu.make_async_copy(part.at[r, pl.ds(0, done)], keep.at[r], ksem.at[n]) for n, r in enumerate(some)]
    outs = [pltpu.make_async_copy(keep.at[r], out_hbm.at[r, pl.ds(0, done)], osem.at[n]) for n, r in enumerate(some)]
    for cp in loads + ins:
        cp.start()
    for cp in loads[:4]:
        cp.wait()
    set_hidden(hid, hs_ref, hb_ref)

    def put(r, v):
        ov[r] = (zv[r].astype(F32) + v).astype(BF)
    hidden_norm(core, lambda i: own_v[:, i // SIDE, i % SIDE].astype(F32), lambda i: par_v[:, i // SIDE, i % SIDE].astype(F32), y, lambda: None)
    for a, b in zip(ins, outs):
        a.wait()
        b.start()
    for cp in loads[4:]:
        cp.wait()
    ends = []
    for n in range(2):
        rows = pl.ds(n * RL // 2, RL // 2)
        out_rows(core, y, hid, wo_ref, wg_ref, lambda r: xv[r], put, n * RL // 2, RL // 2)
        ends.append(pltpu.make_async_copy(ov.at[rows], out_hbm.at[rows, cols, :], osem.at[PASS + n]))
        ends[-1].start()
    for cp in outs + ends:
        cp.wait()


def update_kernel(z_hbm, *refs):
    small, refs = refs[:11], refs[11:]
    (out_hbm, own_out, par_out, x_out, mask_ref, scale_ref, bias_ref, wa_ref, wag_ref, wb_ref, wbg_ref, wg_ref, wo_ref, hs_ref, hb_ref,
                  zbuf, xall, mall, wt, stage_a, stage_b, sa, sb, r1a, r1b, r2a, r2b, aa, bb, y, obuf, hid,
                  zsem, xssem, xown, xmix, mrsem, msem, ssem, rsem, lsem, dssem, drsem, osem, credit, wsem) = refs
    core, coords = place()
    barrier = pltpu.get_barrier_semaphore()
    greet(barrier, core, coords)
    partner = dev(coords, 1 - core)
    ring = [[((coords[d] + by) % SIDE, dev(shift(coords, d, by), core)) for by in (1, 3, 2)] for d in range(3)]
    own0, mix0 = 4 * core, 8 - 8 * core
    tile = [s + core * (2 - 2 * s) for s in range(NG)]
    full = slice(None)

    def qcols(q):
        return pl.ds(q * KQ, KQ)

    first = [u for u in UNITS if u[0] == 0]
    loads = [pltpu.make_async_copy(z_hbm.at[pl.ds(own0, TR), pl.ds(at, w)], zbuf.at[pl.ds(own0, TR), pl.ds(at, w)], zsem.at[n])
             for n, (_, at, w) in enumerate(first)]
    loads.append(pltpu.make_async_copy(z_hbm.at[pl.ds(mix0, 4)], zbuf.at[pl.ds(mix0, 4)], zsem.at[len(first)]))
    held = (mask_ref, scale_ref, bias_ref, wa_ref, wag_ref, wb_ref, wbg_ref, wg_ref, wo_ref, hs_ref, hb_ref)
    copies = [pltpu.make_async_copy(a, b, wsem.at[n]) for n, (a, b) in enumerate(zip(small, held))]
    loads[0].start()
    for cp in copies:
        cp.start()
    for cp in copies:
        cp.wait()
    for cp in loads[1:]:
        cp.start()
    for i, w in enumerate((wa_ref, wag_ref, wb_ref, wbg_ref)):
        wt[i] = w[...].astype(F32).T.astype(BF)
    mall[core] = mask_ref[...]
    scale = scale_ref[...].astype(F32)
    bias = bias_ref[...].astype(F32)
    half = pl.ds(pl.multiple_of(core * CH, CH), CH)
    wcat = jnp.concatenate([wt[i, half, :] for i in range(4)], axis=0)

    average = jnp.full((C, C), 1.0 / C, BF)

    def norm(row0, rows, start, width):
        def body(i, carry):
            r = row0 + i
            for k in range(width // KC):
                at = pl.ds(start + k * KC, KC)
                v = zbuf[r, at, :]
                centered = v.astype(F32) - jnp.dot(v, average, preferred_element_type=F32)
                var = jnp.mean(centered * centered, axis=-1, keepdims=True)
                xall[core * RL + r, at, :] = (centered * lax.rsqrt(var + LN_EPS) * scale + bias).astype(BF)
            return carry
        lax.fori_loop(0, rows, body, 0, unroll=8 if width == KC else 1)

    def give_x(row0, rows, start, width, sem):
        block = xall.at[pl.ds(core * RL + row0, rows), pl.ds(start, width)]
        pltpu.make_async_remote_copy(src_ref=block, dst_ref=block, send_sem=xssem, recv_sem=sem,
                                     device_id=partner, device_id_type=MESH).start()

    bufs = ((sb, r1b, r2b), (sa, r1a, r2a))

    def unit_sem(arr, n, ph):
        if ph < 2:
            return rsem.at[arr, n, ph]
        return lsem.at[NG] if arr == 0 else lsem.at[UNITS[n][0]]

    def phase(arr, n, ph):
        s, start, width = UNITS[n]
        cols = pl.ds(start, width)
        dim = (n + arr + ph) % 3
        src = bufs[arr][ph]

        def at(p):
            return (s,) + p + (full, cols)

        def final(p):
            return p + (tile[s], full, cols) if arr == 0 else at(p)
        dst = (bb, aa)[arr] if ph == 2 else bufs[arr][ph + 1]
        dst_at = final if ph == 2 else at
        send_phase(ring, coords, dim, lambda p: src.at[at(p)], lambda p: dst.at[dst_at(p)], ssem.at[arr, ph],
                   unit_sem(arr, n, ph))
        keep_own(coords, dim, src, at, dst, dst_at)

    def arrived(arr, n, ph):
        s, start, width = UNITS[n]
        wait_bytes(r1a.at[s, pl.ds(0, 3), full, full, full, pl.ds(start, width)], rsem.at[arr, n, ph])

    def make_unit(n):
        s, start, width = UNITS[n]

        def project_row(i, carry):
            row = tile[s] * TR + i
            owner, within = row // RL, row % RL
            for j in range(width // KC):
                at = pl.ds(start + j * KC, KC)
                p = lax.dot_general(wcat, xall[row, at, :], (((1,), (1,)), ((), ())), preferred_element_type=F32)
                keep = mall[owner, pl.ds(within, 1), at].astype(F32)
                a = sigmoid(p[CH:2 * CH]) * p[:CH] * keep
                b = sigmoid(p[3 * CH:]) * p[2 * CH:3 * CH] * keep
                for u in range(KC // 128):
                    lanes = slice(u * 128, (u + 1) * 128)
                    kt = j * (KC // 128) + u
                    stage_a[kt, pl.ds(i, CH, stride=SKEW), :] = a[:, lanes]
                    stage_b[kt, pl.ds(i, CH, stride=SKEW), :] = b[:, lanes]
            return carry
        lax.fori_loop(0, TR, project_row, 0, unroll=8 if width == KC else 4)
        for arr, stage in ((0, stage_b), (1, stage_a)):
            s_ref = bufs[arr][0]

            def pack(i):
                def pack_y(k):
                    def pack_x(m):
                        c = (i * SIDE + k) * SIDE + m
                        for j in range(width // KC):
                            v = jnp.concatenate([stage[2 * j + u, pl.ds(c * SKEW, TR), :] for u in range(2)], axis=1)
                            s_ref[s, i, k, m, :, pl.ds(start + j * KC, KC)] = v.astype(BF)
                    loop(SIDE, pack_x, unroll=SIDE)
                loop(SIDE, pack_y)
            loop(SIDE, pack)
            phase(arr, n, 0)

    def forward(arr, n, ph):
        arrived(arr, n, ph - 1)
        phase(arr, n, ph)

    for n, (s, start, width) in enumerate(UNITS):
        if s == 0:
            loads[n].wait()
            norm(own0, TR, start, width)
            if n == 0:
                pl.semaphore_wait(barrier, GREETED)
                mcopy = pltpu.make_async_remote_copy(src_ref=mask_ref, dst_ref=mall.at[core], send_sem=msem, recv_sem=mrsem,
                                                     device_id=partner, device_id_type=MESH)
                mcopy.start()
            give_x(own0, TR, start, width, xown.at[n])
        if n == len(first):
            mcopy.wait()
            for k, (_, at, w) in enumerate(first):
                wait_bytes(xall.at[pl.ds(0, TR), pl.ds(at, w)], xown.at[k])
        if n == len(first) + 1:
            loads[len(first)].wait()
            norm(mix0, 4, 0, N)
            give_x(mix0, 4, 0, N, xmix)
        if s == 1 and start == 0:
            wait_bytes(xall.at[pl.ds(0, 4)], xmix)
        make_unit(n)

    for n in range(len(UNITS)):
        forward(0, n, 1)
        forward(1, n, 1)
    for arr in range(2):
        for n in range(len(UNITS)):
            forward(arr, n, 2)
    for arr, ph in ((0, 0), (1, 0), (0, 1), (1, 1), (0, 2)):
        wait_bytes(r1a.at[:, pl.ds(0, 3)], ssem.at[arr, ph])
    wait_bytes(r1a.at[:, pl.ds(0, 3)], lsem.at[NG])
    greet(credit, core, coords)
    wait_bytes(zbuf, xssem)

    x_copy = pltpu.make_async_copy(xall.at[pl.ds(core * RL, RL), qcols(NQ - 1)], x_out, msem)
    x_copy.start()
    set_hidden(hid, hs_ref, hb_ref)

    def part_sem(s, q, ph):
        k = 2 * NG * NQ + q if ph == 2 else (s * NQ + q) * 2 + ph
        return rsem.at[k // (2 * len(UNITS)), (k // 2) % len(UNITS), k % 2]

    def tphase(s, q, ph):
        dim = (s + q + ph) % 3
        src = (sb, r1b, r2b)[ph]
        dst = (r1b, r2b, sa)[ph]

        def at(p):
            return (s,) + p + (full, qcols(q))

        def final(p):
            return (tile[s],) + p + (full, qcols(q))
        dst_at = final if ph == 2 else at
        send_phase(ring, coords, dim, lambda p: src.at[at(p)], lambda p: dst.at[dst_at(p)], ssem.at[0, ph], part_sem(s, q, ph))
        keep_own(coords, dim, src, at, dst, dst_at)

    def tarrived(s, q, ph):
        wait_bytes(r1b.at[s, pl.ds(0, 3), full, full, full, qcols(q)], part_sem(s, q, ph))

    order = [s for s, _ in PARTS]
    slab = N // SIDE
    for s in order:
        wait_bytes(r1a.at[s, pl.ds(0, 3)], lsem.at[s])
        for k in range(SIDE):
            acc = lax.dot_general(aa[s].reshape(CH * TR, N), bb[k].reshape(slab, N), (((1,), (1,)), ((), ())),
                                  preferred_element_type=F32)
            sb[s, :, :, :, :, pl.ds(k * slab, slab)] = acc.astype(BF).reshape(SIDE, SIDE, SIDE, TR, slab)
            if s == order[0] and k == 0:
                pl.semaphore_wait(credit, GREETED)
            for q in range(NQ):
                if k * slab < (q + 1) * KQ <= (k + 1) * slab:
                    tphase(s, q, 0)
    for ph in (1, 2):
        for q in range(NQ):
            for s in order:
                tarrived(s, q, ph - 1)
                tphase(s, q, ph)

    def swap(q):
        return pltpu.make_async_remote_copy(
            src_ref=sa.at[pl.ds(1 - core, 2), :, :, :, :, qcols(q)],
            dst_ref=r1a.at[pl.ds(0, 2), :, :, :, :, qcols(q)] if q < NQ - 1 else par_out,
            send_sem=dssem, recv_sem=drsem.at[q], device_id=partner, device_id_type=MESH)

    def store(q):
        return pltpu.make_async_copy(obuf.at[q % 2], out_hbm.at[:, qcols(q), :], osem.at[q])

    def finish(q):
        def own(i):
            return sa[pl.ds(core, 2), i // SIDE, i % SIDE, :, :, qcols(q)].astype(F32)

        def par(i):
            return r1a[pl.ds(0, 2), i // SIDE, i % SIDE, :, :, qcols(q)].astype(F32)

        def put(r, v):
            obuf[q % 2, r] = (zbuf[r, qcols(q), :].astype(F32) + v).astype(BF)
        hidden_norm(core, own, par, y, lambda: ready(q + 1))
        out_rows(core, y, hid, wo_ref, wg_ref, lambda r: xall[core * RL + r, qcols(q), :], put)

    def ready(q):
        wait_bytes(r1b.at[:, pl.ds(0, 3), full, full, full, qcols(q)], part_sem(0, q, 2))
        swap(q).start()
        if q == NQ - 1:
            own_copy.start()

    own_copy = pltpu.make_async_copy(sa.at[pl.ds(core, 2), :, :, :, :, qcols(NQ - 1)], own_out, osem.at[NQ - 1])
    ready(0)
    for q in range(NQ - 1):
        swap(q).wait_recv()
        if q >= 2:
            store(q - 2).wait()
        finish(q)
        store(q).start()
    wait_bytes(sa.at[pl.ds(0, 2)], dssem)
    for ph in range(3):
        wait_bytes(r1a.at[:, pl.ds(0, 3)], ssem.at[0, ph])
    wait_bytes(r1a.at[:, pl.ds(0, 3)], ssem.at[1, 2])
    x_copy.wait()
    store(NQ - 3).wait()
    store(NQ - 2).wait()
    own_copy.wait()
    swap(NQ - 1).wait_recv()


def solution(mesh):
    row_spec = P(('data', 'dap'), None, None)
    mask_spec = P(('data', 'dap'), None)
    replicated = P()
    aspec = pl.BlockSpec(memory_space=ANY)

    def local_fn(z_loc, mask_loc, ln_scale, ln_bias, w_a, w_a_gate, w_b, w_b_gate, w_gate, ln_hid_scale, ln_hid_bias, w_out):
        sets = VMEM((NG, SIDE, SIDE, SIDE, TR, N), BF)
        line, square = VMEM((1, C), BF), VMEM((C, C), BF)
        edge = jax.ShapeDtypeStruct((2, SIDE, SIDE, SIDE, TR, KQ), BF)
        hs, hb = ln_hid_scale.reshape(1, C), ln_hid_bias.reshape(1, C)
        part, own, par, x_last = pl.pallas_call(
            update_kernel, name='update',
            out_shape=(jax.ShapeDtypeStruct((RL, N, C), BF), edge, edge, jax.ShapeDtypeStruct((RL, KQ, C), BF)),
            in_specs=[aspec] * 12, out_specs=(aspec,) * 4,
            scratch_shapes=[VMEM((RL, N), jnp.int32), line, line] + [square] * 6 + [line] * 2 + [
                VMEM((RL, N, C), BF), VMEM((2 * RL, N, C), BF), VMEM((2, RL, N), jnp.int32), VMEM((4, C, C), BF),
                VMEM((KT // 128, CH * SKEW + 16, 128), F32), VMEM((KT // 128, CH * SKEW + 16, 128), F32),
                sets, sets, sets, sets, sets, sets, sets, VMEM((SIDE, SIDE, SIDE, NG, TR, N), BF),
                VMEM((KQ // 128, (2 * TR + 1) * YSK + 7, 128), F32), VMEM((2, RL, KQ, C), BF), VMEM((2, C, C), F32),
                DMA((N // PARTS[0][1] + 1,)), DMA, DMA((N // PARTS[0][1],)), DMA, DMA, DMA, DMA((2, 3)), DMA((2, len(UNITS), 2)),
                DMA((NG + 1,)), DMA, DMA((NQ,)), DMA((NQ,)), pltpu.SemaphoreType.REGULAR, DMA((11,))],
            compiler_params=pltpu.CompilerParams(collective_id=1, has_side_effects=True, vmem_limit_bytes=67043328),
        )(z_loc, mask_loc, ln_scale.reshape(1, C), ln_bias.reshape(1, C), w_a, w_a_gate, w_b, w_b_gate, w_gate, w_out, hs, hb)
        edge_v = VMEM((2, SIDE, SIDE, SIDE, TR, KQ), BF)
        block = VMEM((RL, KQ, C), BF)
        return pl.pallas_call(
            last_kernel, name='last', out_shape=jax.ShapeDtypeStruct((RL, N, C), BF),
            in_specs=[aspec] * 9, out_specs=aspec,
            scratch_shapes=[VMEM((RL, N - KQ, C), BF), edge_v, edge_v, block, block, square, square, line, line, block,
                            VMEM((KQ // 128, (2 * TR + 1) * YSK + 7, 128), F32), VMEM((2, C, C), F32), DMA((8,)), DMA((PASS,)), DMA((PASS + 2,))],
            compiler_params=pltpu.CompilerParams(vmem_limit_bytes=60 * 2**20),
        )(part, own, par, x_last, z_loc, w_gate, w_out, hs, hb)

    return jax.shard_map(local_fn, mesh=mesh, in_specs=(row_spec, mask_spec) + (replicated,) * 10, out_specs=row_spec, check_vma=False)
```
